128 devices in a mesh: data: 32 (over z, y, x_hi), width: 4 (over x_lo, core).
Axes of the slice: x: 4 (x_hi: 2, x_lo: 2; x = x_hi * 2 + x_lo), y: 4, z: 4, core: 2. Of those that a mesh axis runs over, the one named last changes fastest.
Arguments:
- grad_up: float32 [32, 768, 3072], P('data', None, 'width'), may hold values from -6 to 6
- grad_down: float32 [32, 3072, 768], P('data', 'width'), may hold values from -6 to 6
- grad_query: float32 [32, 768, 768], P('data', None, 'width'), may hold values from -6 to 6
- grad_key: float32 [32, 768, 768], P('data', None, 'width'), may hold values from -6 to 6
- grad_value: float32 [32, 768, 768], P('data', None, 'width'), may hold values from -6 to 6
- grad_mixed: float32 [32, 768, 768], P('data', 'width'), may hold values from -6 to 6
- grad_norm: float32 [32, 768], P('data'), may hold values from -12 to 12
- weight_up: float32 [768, 3072], P('data', 'width'), may hold values from -0.21875 to 0.21875
- weight_down: float32 [3072, 768], P('width', 'data'), may hold values from -0.109375 to 0.109375
- weight_query: float32 [768, 768], P('data', 'width'), may hold values from -0.21875 to 0.21875
- weight_key: float32 [768, 768], P('data', 'width'), may hold values from -0.21875 to 0.21875
- weight_value: float32 [768, 768], P('data', 'width'), may hold values from -0.21875 to 0.21875
- weight_mixed: float32 [768, 768], P('width', 'data'), may hold values from -0.21875 to 0.21875
- weight_norm: float32 [768], P('data'), may hold values from 0.25 to 1.75
- moment_up: float32 [768, 3072], P('data', 'width'), may hold values from 0.05 to 0.8
- moment_down: float32 [3072, 768], P('width', 'data'), may hold values from 0.05 to 0.8
- moment_query: float32 [768, 768], P('data', 'width'), may hold values from 0.05 to 0.8
- moment_key: float32 [768, 768], P('data', 'width'), may hold values from 0.05 to 0.8
- moment_value: float32 [768, 768], P('data', 'width'), may hold values from 0.05 to 0.8
- moment_mixed: float32 [768, 768], P('width', 'data'), may hold values from 0.05 to 0.8
- moment_norm: float32 [768], P('data'), may hold values from 0.05 to 0.8
Outputs:
- copy_up: bfloat16 [768, 3072], P(None, 'width')
- copy_down: bfloat16 [3072, 768], P('width')
- copy_query: bfloat16 [768, 768], P(None, 'width')
- copy_key: bfloat16 [768, 768], P(None, 'width')
- copy_value: bfloat16 [768, 768], P(None, 'width')
- copy_mixed: bfloat16 [768, 768], P('width')
- copy_norm: bfloat16 [768], replicated
- new_up: float32 [768, 3072], P('data', 'width')
- new_down: float32 [3072, 768], P('width', 'data')
- new_query: float32 [768, 768], P('data', 'width')
- new_key: float32 [768, 768], P('data', 'width')
- new_value: float32 [768, 768], P('data', 'width')
- new_mixed: float32 [768, 768], P('width', 'data')
- new_norm: float32 [768], P('data')
- state_new_up: float32 [768, 3072], P('data', 'width')
- state_new_down: float32 [3072, 768], P('width', 'data')
- state_new_query: float32 [768, 768], P('data', 'width')
- state_new_key: float32 [768, 768], P('data', 'width')
- state_new_value: float32 [768, 768], P('data', 'width')
- state_new_mixed: float32 [768, 768], P('width', 'data')
- state_new_norm: float32 [768], P('data')
The draws below stay inside these ranges and needn't reach their ends.
All inputs are finite; a program needn't handle non-finite values.
Results may differ from the reference program's by a relative error of at most 0.0004.
Values may be sent and summed in bfloat16 or wider, within the bound.
A program may use at most 128 MiB of HBM per device.

```python
import jax
import jax.numpy as jnp
from jax import lax

WIDTH = 768
INNER = 3072
ATTN = 768
REPLICAS = 32


def raised(entries, stream_key, source, target, parts, factor):
    owner, partner = [(jnp.arange(entries.shape[axis_at]) // (entries.shape[axis_at] // parts)).reshape([-1 if axis == axis_at else 1 for axis in range(entries.ndim)]) for axis_at in (source, target)]
    chosen = jax.random.permutation(stream_key, parts)[partner]
    strong = (owner == chosen) | (owner == (partner + parts // 2) % parts)
    return jnp.where(strong, factor * entries, entries)


def block_scale(key, dims, split, smallest, largest):
    def one(dim, shards_of):
        draws = jax.random.uniform(jax.random.fold_in(jax.random.fold_in(key, 6), dim), (shards_of,), jnp.float32, smallest / len(split), largest / len(split))
        return jnp.repeat(jnp.exp(draws), dims[dim] // shards_of).reshape((-1,) + (1,) * (len(dims) - dim - 1))

    loudness = one(*split[0])
    for cut in split[1:]:
        loudness = loudness * one(*cut)
    return loudness


def scatter_about(own_key, extent, deviation, reach, split=(), held_as=jnp.bfloat16):
    factor_of = block_scale(own_key, extent, split, -0.22, 0.18) if split else 1.0
    drawn = jax.random.normal(own_key, extent, jnp.float32) * deviation * factor_of
    return jnp.minimum(jnp.maximum(drawn, -reach), reach).astype(held_as)


def noise_with(rng, dims, width, reach, pieces, heavy, kind=jnp.bfloat16):
    drawn = width * jax.random.normal(rng, dims, jnp.float32)
    if pieces:
        drawn = drawn * block_scale(rng, dims, pieces, -0.22, 0.18)
    return jnp.clip(raised(drawn, jax.random.fold_in(rng, 3), *heavy), -reach, reach).astype(kind)


def setup_inputs(seed: int = 0) -> dict:
    keys = jax.random.split(jax.random.key(seed), 22)
    grad_up = noise_with(keys[0], (REPLICAS, WIDTH, INNER), 0.5, 6.0, ((0, 32), (2, 4)), (0, 1, 32, 2.75), jnp.float32)
    grad_down = noise_with(keys[1], (REPLICAS, INNER, WIDTH), 0.5, 6.0, ((0, 32), (1, 4)), (0, 2, 32, 2.75), jnp.float32)
    grad_query = noise_with(keys[2], (REPLICAS, WIDTH, ATTN), 0.5, 6.0, ((0, 32), (2, 4)), (0, 1, 32, 2.75), jnp.float32)
    grad_key = noise_with(keys[3], (REPLICAS, WIDTH, ATTN), 0.5, 6.0, ((0, 32), (2, 4)), (0, 1, 32, 2.75), jnp.float32)
    grad_value = noise_with(keys[4], (REPLICAS, WIDTH, ATTN), 0.5, 6.0, ((0, 32), (2, 4)), (0, 1, 32, 2.75), jnp.float32)
    grad_mixed = noise_with(keys[5], (REPLICAS, ATTN, WIDTH), 0.5, 6.0, ((0, 32), (1, 4)), (0, 2, 32, 2.75), jnp.float32)
    grad_norm = noise_with(keys[6], (REPLICAS, WIDTH), 1.0, 12.0, ((0, 32),), (0, 1, 32, 2.75), jnp.float32)
    weight_up = scatter_about(keys[7], (WIDTH, INNER), WIDTH ** -0.5, 0.21875, ((0, 32), (1, 4)), jnp.float32)
    weight_down = scatter_about(keys[8], (INNER, WIDTH), INNER ** -0.5, 0.109375, ((0, 4), (1, 32)), jnp.float32)
    weight_query = scatter_about(keys[9], (WIDTH, ATTN), WIDTH ** -0.5, 0.21875, ((0, 32), (1, 4)), jnp.float32)
    weight_key = scatter_about(keys[10], (WIDTH, ATTN), WIDTH ** -0.5, 0.21875, ((0, 32), (1, 4)), jnp.float32)
    weight_value = scatter_about(keys[11], (WIDTH, ATTN), WIDTH ** -0.5, 0.21875, ((0, 32), (1, 4)), jnp.float32)
    weight_mixed = scatter_about(keys[12], (ATTN, WIDTH), ATTN ** -0.5, 0.21875, ((0, 4), (1, 32)), jnp.float32)
    weight_norm = jnp.clip(1.0 + 0.15 * jax.random.normal(keys[13], (WIDTH,), jnp.float32), 0.25, 1.75)
    moment_up = jnp.clip(0.05 + 0.75 * jax.random.uniform(keys[14], (WIDTH, INNER), jnp.float32) ** block_scale(keys[14], (WIDTH, INNER), ((0, 32), (1, 4)), -0.2, 0.2), 0.05, 0.8)
    moment_down = jnp.clip(0.05 + 0.75 * jax.random.uniform(keys[15], (INNER, WIDTH), jnp.float32) ** block_scale(keys[15], (INNER, WIDTH), ((0, 4), (1, 32)), -0.2, 0.2), 0.05, 0.8)
    moment_query = jnp.clip(0.05 + 0.75 * jax.random.uniform(keys[16], (WIDTH, ATTN), jnp.float32) ** block_scale(keys[16], (WIDTH, ATTN), ((0, 32), (1, 4)), -0.2, 0.2), 0.05, 0.8)
    moment_key = jnp.clip(0.05 + 0.75 * jax.random.uniform(keys[17], (WIDTH, ATTN), jnp.float32) ** block_scale(keys[17], (WIDTH, ATTN), ((0, 32), (1, 4)), -0.2, 0.2), 0.05, 0.8)
    moment_value = jnp.clip(0.05 + 0.75 * jax.random.uniform(keys[18], (WIDTH, ATTN), jnp.float32) ** block_scale(keys[18], (WIDTH, ATTN), ((0, 32), (1, 4)), -0.2, 0.2), 0.05, 0.8)
    moment_mixed = jnp.clip(0.05 + 0.75 * jax.random.uniform(keys[19], (ATTN, WIDTH), jnp.float32) ** block_scale(keys[19], (ATTN, WIDTH), ((0, 4), (1, 32)), -0.2, 0.2), 0.05, 0.8)
    moment_norm = jnp.clip(0.05 + 0.75 * jax.random.uniform(keys[20], (WIDTH,), jnp.float32) ** block_scale(keys[20], (WIDTH,), ((0, 32),), -0.2, 0.2), 0.05, 0.8)
    return dict(grad_up=grad_up, grad_down=grad_down, grad_query=grad_query, grad_key=grad_key, grad_value=grad_value, grad_mixed=grad_mixed, grad_norm=grad_norm, weight_up=weight_up, weight_down=weight_down, weight_query=weight_query, weight_key=weight_key, weight_value=weight_value, weight_mixed=weight_mixed, weight_norm=weight_norm, moment_up=moment_up, moment_down=moment_down, moment_query=moment_query, moment_key=moment_key, moment_value=moment_value, moment_mixed=moment_mixed, moment_norm=moment_norm)


learn_rate = 0.05
hold_rate = 0.9

def reference(grad_up, grad_down, grad_query, grad_key, grad_value, grad_mixed, grad_norm, weight_up, weight_down, weight_query, weight_key, weight_value, weight_mixed, weight_norm, moment_up, moment_down, moment_query, moment_key, moment_value, moment_mixed, moment_norm):
    mean_up = lax.optimization_barrier(jnp.sum(grad_up.astype(jnp.float32), axis=0)) * REPLICAS ** (-0.5)
    mean_down = lax.optimization_barrier(jnp.sum(grad_down.astype(jnp.float32), axis=0)) * REPLICAS ** (-0.5)
    mean_query = lax.optimization_barrier(jnp.sum(grad_query.astype(jnp.float32), axis=0)) * REPLICAS ** (-0.5)
    mean_key = lax.optimization_barrier(jnp.sum(grad_key.astype(jnp.float32), axis=0)) * REPLICAS ** (-0.5)
    mean_value = lax.optimization_barrier(jnp.sum(grad_value.astype(jnp.float32), axis=0)) * REPLICAS ** (-0.5)
    mean_mixed = lax.optimization_barrier(jnp.sum(grad_mixed.astype(jnp.float32), axis=0)) * REPLICAS ** (-0.5)
    mean_norm = lax.optimization_barrier(jnp.sum(grad_norm.astype(jnp.float32), axis=0)) * REPLICAS ** (-0.5)
    state_new_up = hold_rate * moment_up + (1.0 - hold_rate) * mean_up * mean_up
    new_up = weight_up - learn_rate * mean_up * lax.rsqrt(state_new_up + 1e-06)
    state_new_down = hold_rate * moment_down + (1.0 - hold_rate) * mean_down * mean_down
    new_down = weight_down - learn_rate * mean_down * lax.rsqrt(state_new_down + 1e-06)
    state_new_query = hold_rate * moment_query + (1.0 - hold_rate) * mean_query * mean_query
    new_query = weight_query - learn_rate * mean_query * lax.rsqrt(state_new_query + 1e-06)
    state_new_key = hold_rate * moment_key + (1.0 - hold_rate) * mean_key * mean_key
    new_key = weight_key - learn_rate * mean_key * lax.rsqrt(state_new_key + 1e-06)
    state_new_value = hold_rate * moment_value + (1.0 - hold_rate) * mean_value * mean_value
    new_value = weight_value - learn_rate * mean_value * lax.rsqrt(state_new_value + 1e-06)
    state_new_mixed = hold_rate * moment_mixed + (1.0 - hold_rate) * mean_mixed * mean_mixed
    new_mixed = weight_mixed - learn_rate * mean_mixed * lax.rsqrt(state_new_mixed + 1e-06)
    state_new_norm = hold_rate * moment_norm + (1.0 - hold_rate) * mean_norm * mean_norm
    new_norm = weight_norm - learn_rate * mean_norm * lax.rsqrt(state_new_norm + 1e-06)
    copy_up = new_up.astype(jnp.bfloat16)
    copy_down = new_down.astype(jnp.bfloat16)
    copy_query = new_query.astype(jnp.bfloat16)
    copy_key = new_key.astype(jnp.bfloat16)
    copy_value = new_value.astype(jnp.bfloat16)
    copy_mixed = new_mixed.astype(jnp.bfloat16)
    copy_norm = new_norm.astype(jnp.bfloat16)
    return (copy_up, copy_down, copy_query, copy_key, copy_value, copy_mixed, copy_norm, new_up, new_down, new_query, new_key, new_value, new_mixed, new_norm, state_new_up, state_new_down, state_new_query, state_new_key, state_new_value, state_new_mixed, state_new_norm)
```

```python
import jax
import jax.numpy as jnp
from jax import lax
from jax.experimental import pallas as pl
from jax.experimental.pallas import tpu as pltpu
from jax.sharding import PartitionSpec as P

learn_rate = 0.05
hold_rate = 0.9
mean_rate = 32 ** (-0.5)

MESH = pl.DeviceIdType.MESH
PIECES = 3
WIDE = 256
HALF = 128
UP, DOWN, MIXED = 0, 1, 2
FOLDED = (4, 4, 2, 24, WIDE)

SENDS = 36 * 3 + 28 * 6 + 7


def on_ring(step, size=4):
    return lax.rem(step, size)


class Place:
    def __init__(self):
        data, width = lax.axis_index("data"), lax.axis_index("width")
        self.z, self.y, self.xh = lax.div(data, 8), lax.rem(lax.div(data, 2), 4), lax.rem(data, 2)
        self.x, self.core = 2 * self.xh + lax.div(width, 2), lax.rem(width, 2)
        self.data = data

    def device(self, z, y, x):
        return (z * 8 + y * 2 + lax.div(x, 2), 2 * lax.rem(x, 2) + self.core)

    def along(self, axis, step):
        z, y, x = self.z, self.y, self.x
        if axis == "z":
            z = on_ring(z + step)
        elif axis == "y":
            y = on_ring(y + step)
        else:
            x = on_ring(x + step)
        return self.device(z, y, x)


class Sender:
    def __init__(self, place, send_sems, recv_sems):
        self.place, self.send_sems, self.recv_sems = place, send_sems, recv_sems
        self.copies = []

    def start(self, source, target, axis, step):
        n = len(self.copies)
        copy = pltpu.make_async_remote_copy(
            src_ref=source,
            dst_ref=target,
            send_sem=self.send_sems.at[n],
            recv_sem=self.recv_sems.at[n],
            device_id=self.place.along(axis, step),
            device_id_type=MESH,
        )
        copy.start()
        self.copies.append(copy)
        return copy

    def finish(self):
        for copy in self.copies:
            copy.wait_send()


def add_to(ref, *others):
    total = ref[...]
    for other in others:
        total = total + other[...]
    ref[...] = total


def ring_scatter(sender, block, axis, at, landing):
    plus, minus = on_ring(at + 1), on_ring(at + 3)
    opposite = on_ring(at + 2)
    far_plus = sender.start(block(opposite, 0), landing.at[0], axis, 1)
    far_minus = sender.start(block(opposite, 1), landing.at[1], axis, 3)
    near_plus = sender.start(block(plus, 1), landing.at[2], axis, 1)
    near_minus = sender.start(block(minus, 0), landing.at[3], axis, 3)
    yield
    far_plus.wait_recv()
    add_to(block(plus, 0), landing.at[0])
    both_plus = sender.start(block(plus, 0), landing.at[4], axis, 1)
    far_minus.wait_recv()
    add_to(block(minus, 1), landing.at[1])
    both_minus = sender.start(block(minus, 1), landing.at[5], axis, 3)
    yield
    near_minus.wait_recv()
    both_plus.wait_recv()
    add_to(block(at, 0), landing.at[3], landing.at[4])
    near_plus.wait_recv()
    both_minus.wait_recv()
    add_to(block(at, 1), landing.at[2], landing.at[5])


def ring_gather(sender, block, axis, at):
    plus, minus = on_ring(at + 1), on_ring(at + 3)
    first_plus = sender.start(block(at, 0), block(at, 0), axis, 1)
    first_minus = sender.start(block(at, 1), block(at, 1), axis, 3)
    second_plus = sender.start(block(at, 1), block(at, 1), axis, 1)
    second_minus = sender.start(block(at, 0), block(at, 0), axis, 3)
    yield
    first_plus.wait_recv()
    on_plus = sender.start(block(minus, 0), block(minus, 0), axis, 1)
    first_minus.wait_recv()
    on_minus = sender.start(block(plus, 1), block(plus, 1), axis, 3)
    yield
    for copy in (second_plus, second_minus, on_plus, on_minus):
        copy.wait_recv()


def updated(mean, weight, moment):
    state = hold_rate * moment + (1.0 - hold_rate) * mean * mean
    return weight - learn_rate * mean * lax.rsqrt(state + 1e-06), state


def stacked(block):
    return jnp.concatenate([block[:, :HALF], block[:, HALF:]], axis=0)


def exchange_kernel(*refs):
    (
        grad_up, grad_down, grad_query, grad_key, grad_value, grad_mixed, grad_norm,
        weight_up, weight_down, weight_query, weight_key, weight_value, weight_mixed, weight_norm,
        moment_up, moment_down, moment_query, moment_key, moment_value, moment_mixed, moment_norm,
        copy_up, copy_down, copy_query, copy_key, copy_value, copy_mixed, kept, norm_out,
        sums, turned, held, held_heads, whole, staged, kept_own, norm_own,
        pair_relay, pair_land, wide_land, thin_land,
        first_land, second_land, own_relay, own_land,
        copy_relay, copy_pair_relay,
        norm_grad, norm_held, norm_rows, norm_pair, norm_ring,
        send_sems, recv_sems, load_sems, store_sems,
    ) = refs
    place = Place()
    z, y, xh, x = place.z, place.y, place.xh, place.x
    far_xh = 1 - xh
    columns = [pl.ds(WIDE * k, WIDE) for k in range(PIECES)]

    loads = {}

    def load(name, source, target):
        copy = pltpu.make_async_copy(source, target, load_sems.at[len(loads)])
        copy.start()
        loads[name] = copy

    heads = (grad_query, grad_key, grad_value, grad_mixed)
    for k in range(PIECES):
        load(("up", k), grad_up.at[:, :, :, :, columns[k]], sums.at[UP, k])
        load(("down", k), grad_down.at[columns[k], :], turned.at[0, columns[k], :])
        for head in ((0, 1), (2,), (3,))[k]:
            load(("head", head), heads[head], turned.at[1, pl.ds(192 * head, 192), :])
    load("norm", grad_norm, norm_grad)
    load("weight_norm", weight_norm, norm_held.at[0])
    load("moment_norm", moment_norm, norm_held.at[1])
    load("weight_up", weight_up, held.at[0, UP])
    load("moment_up", moment_up, held.at[1, UP])
    load("weight_down", weight_down, held.at[0, DOWN])
    load("moment_down", moment_down, held.at[1, DOWN])
    for head, source in enumerate((weight_query, weight_key, weight_value, weight_mixed)):
        load(("weight", head), source, held_heads.at[0, head])
    for head, source in enumerate((moment_query, moment_key, moment_value, moment_mixed)):
        load(("moment", head), source, held_heads.at[1, head])

    barrier = pltpu.get_barrier_semaphore()
    for axis in ("x", "y", "z"):
        for step in (1, 2, 3):
            pl.semaphore_signal(barrier, inc=1, device_id=place.along(axis, step), device_id_type=MESH)
    pl.semaphore_wait(barrier, 9)

    sender = Sender(place, send_sems, recv_sems)
    stores = []

    def store(source, target):
        copy = pltpu.make_async_copy(source, target, store_sems.at[len(stores)])
        copy.start()
        stores.append(copy)

    def update_piece(part, k):
        own = sums[part, k, z, y, xh] * mean_rate
        new, state = updated(own, held[0, part, :, columns[k]], held[1, part, :, columns[k]])
        kept_own[0, part, :, columns[k]] = new
        kept_own[1, part, :, columns[k]] = state
        whole[part, k, z, y, xh] = stacked(new).astype(jnp.bfloat16)

    def up_stream(k):
        block = sums.at[UP, k]
        copied = whole.at[UP, k]
        second, third = ("y", "z") if k % 2 == 0 else ("z", "y")
        loads["up", k].wait()
        sent = [
            sender.start(block.at[pl.ds(2 * h, 2), :, far_xh], pair_relay.at[k, h], "x", (1, 3)[h])
            for h in range(2)
        ]
        yield
        on = []
        for h in range(2):
            sent[h].wait_recv()
            on.append(sender.start(pair_relay.at[k, h], pair_land.at[k, h], "x", (1, 3)[h]))
        yield
        for h in range(2):
            on[h].wait_recv()
            add_to(block.at[pl.ds(2 * h, 2), :, xh], pair_land.at[k, h])
        if second == "y":
            yield from ring_scatter(
                sender, lambda q, h: block.at[pl.ds(2 * h, 2), q, xh], "y", y, wide_land.at[k]
            )
            yield from ring_scatter(
                sender, lambda q, h: block.at[q, y, xh, :, pl.ds(HALF * h, HALF)], "z", z, thin_land.at[k]
            )
        else:
            yield from ring_scatter(
                sender, lambda q, h: block.at[q, pl.ds(2 * h, 2), xh], "z", z, wide_land.at[k]
            )
            yield from ring_scatter(
                sender, lambda q, h: block.at[z, q, xh, :, pl.ds(HALF * h, HALF)], "y", y, thin_land.at[k]
            )
        if k == 0:
            loads["weight_up"].wait()
            loads["moment_up"].wait()
        update_piece(UP, k)
        rows = (pl.ds(0, 32), pl.ds(32, 16))
        if second == "y":
            yield from ring_gather(sender, lambda q, h: copied.at[q, y, xh, rows[h], :], "z", z)
            yield from ring_gather(sender, lambda q, h: copied.at[pl.ds(2 * h, 2), q, xh], "y", y)
        else:
            yield from ring_gather(sender, lambda q, h: copied.at[z, q, xh, rows[h], :], "y", y)
            yield from ring_gather(sender, lambda q, h: copied.at[q, pl.ds(2 * h, 2), xh], "z", z)
        sent = [
            sender.start(copied.at[pl.ds(2 * h, 2), :, xh], copy_pair_relay.at[k, h], "x", (1, 3)[h])
            for h in range(2)
        ]
        yield
        on = []
        for h in range(2):
            sent[h].wait_recv()
            origin = lax.div(on_ring(x + (3, 1)[h]), 2)
            on.append(
                sender.start(
                    copy_pair_relay.at[k, h], copied.at[pl.ds(2 * h, 2), :, origin], "x", (1, 3)[h]
                )
            )
        yield
        for h in range(2):
            on[h].wait_recv()

        def pair_of_chunks(n, carry):
            chunks = [
                copied[lax.div(n, 4), lax.rem(n, 4), side].astype(jnp.float32) for side in range(2)
            ]
            at = pl.ds(pl.multiple_of(48 * n, 16), 48)
            for half in range(2):
                both = jnp.concatenate([c[24 * half : 24 * half + 24] for c in chunks], axis=0)
                staged[UP, at, pl.ds(WIDE * k + HALF * half, HALF)] = both.astype(jnp.bfloat16)
            return carry

        lax.fori_loop(0, 16, pair_of_chunks, 0)
        store(staged.at[UP, :, columns[k]], copy_up.at[:, columns[k]])

    def turned_stream(part, k):
        block = sums.at[part, k]
        copied = whole.at[part, k]
        step = (1, 3)[part - 1]
        if part == DOWN:
            loads["down", k].wait()
        else:
            for head in ((0, 1), (2,), (3,))[k]:
                loads["head", head].wait()

        def turn(n, carry):
            lanes = pl.ds(pl.multiple_of(384 * n, HALF), 384)
            tile = turned[part - 1, columns[k], lanes]
            block[pl.ds(2 * n, 2)] = tile.T.reshape(2, 4, 2, 24, WIDE)
            return carry

        lax.fori_loop(0, 2, turn, 0)
        if part == DOWN:
            yield from ring_scatter(
                sender, lambda q, h: block.at[q, pl.ds(2 * h, 2)], "z", z, first_land.at[part - 1, k]
            )
            yield from ring_scatter(
                sender, lambda q, h: block.at[z, q, h], "y", y, second_land.at[part - 1, k]
            )
        else:
            yield from ring_scatter(
                sender, lambda q, h: block.at[pl.ds(2 * h, 2), q], "y", y, first_land.at[part - 1, k]
            )
            yield from ring_scatter(
                sender, lambda q, h: block.at[q, y, h], "z", z, second_land.at[part - 1, k]
            )
        sent = sender.start(block.at[z, y, far_xh], own_relay.at[part - 1, k], "x", step)
        yield
        sent.wait_recv()
        on = sender.start(own_relay.at[part - 1, k], own_land.at[part - 1, k], "x", step)
        yield
        on.wait_recv()
        add_to(block.at[z, y, xh], own_land.at[part - 1, k])
        if k == 0:
            if part == DOWN:
                loads["weight_down"].wait()
                loads["moment_down"].wait()
            else:
                for row, name in enumerate(("weight", "moment")):
                    for head in range(4):
                        loads[name, head].wait()
                    held[row, part] = jnp.concatenate([held_heads[row, head] for head in range(4)], axis=1)
        update_piece(part, k)
        sent = sender.start(copied.at[z, y, xh], copy_relay.at[part - 1, k], "x", step)
        yield
        sent.wait_recv()
        origin = lax.div(on_ring(x + 4 - step), 2)
        on = sender.start(copy_relay.at[part - 1, k], copied.at[z, y, origin], "x", step)
        yield
        on.wait_recv()
        if part == DOWN:
            yield from ring_gather(sender, lambda q, h: copied.at[z, q, h], "y", y)
            yield from ring_gather(sender, lambda q, h: copied.at[q, pl.ds(2 * h, 2)], "z", z)
        else:
            yield from ring_gather(sender, lambda q, h: copied.at[q, y, h], "z", z)
            yield from ring_gather(sender, lambda q, h: copied.at[pl.ds(2 * h, 2), q], "y", y)
        for half in range(2):
            tile = copied[:, :, :, 24 * half : 24 * half + 24, :].astype(jnp.float32)
            staged[part, WIDE * k + HALF * half : WIDE * k + HALF * half + HALF, :] = (
                tile.reshape(768, HALF).T.astype(jnp.bfloat16)
            )
        if part == DOWN:
            store(staged.at[DOWN, columns[k], :], copy_down.at[columns[k], :])
        else:
            for head in ((0,), (1,), (2, 3))[k]:
                store(
                    staged.at[MIXED, pl.ds(192 * head, 192), :],
                    (copy_query, copy_key, copy_value, copy_mixed)[head],
                )

    def norm_stream():
        for name in ("norm", "weight_norm", "moment_norm"):
            loads[name].wait()
        norm_rows[...] = jnp.zeros_like(norm_rows)
        norm_rows[1:2, 0:24] = norm_held[0]
        norm_rows[2:3, 0:24] = norm_held[1]
        placed = pltpu.roll(norm_rows[...], 24 * place.data, 1)
        row = lax.broadcasted_iota(jnp.int32, (8, 768), 0)
        norm_pair[xh] = jnp.where(row == 0, jnp.broadcast_to(norm_grad[...], (8, 768)), placed)
        copy = sender.start(norm_pair.at[xh], norm_pair.at[xh], "x", 2)
        yield
        copy.wait_recv()
        norm_ring[0, y] = norm_pair[0] + norm_pair[1]
        copies = [sender.start(norm_ring.at[0, y], norm_ring.at[0, y], "y", s) for s in (1, 2, 3)]
        yield
        for copy in copies:
            copy.wait_recv()
        norm_ring[1, z] = norm_ring[0, 0] + norm_ring[0, 1] + norm_ring[0, 2] + norm_ring[0, 3]
        copies = [sender.start(norm_ring.at[1, z], norm_ring.at[1, z], "z", s) for s in (1, 2, 3)]
        yield
        for copy in copies:
            copy.wait_recv()
        total = norm_ring[1, 0] + norm_ring[1, 1] + norm_ring[1, 2] + norm_ring[1, 3]
        new, state = updated(total[0:1] * mean_rate, total[1:2], total[2:3])
        norm_rows[0:1] = new
        norm_rows[1:2] = state
        norm_own[0] = norm_rows[...]
        norm_own[1] = pltpu.roll(norm_rows[...], lax.rem(768 - 24 * place.data, 768), 1)
        store(norm_own, norm_out)

    streams = {}
    for k in range(PIECES):
        streams[UP, k] = up_stream(k)
        streams[DOWN, k] = turned_stream(DOWN, k)
        streams[MIXED, k] = turned_stream(MIXED, k)
    streams["norm"] = norm_stream()
    for name in ORDER:
        next(streams[name], None)
    store(kept_own, kept)
    for copy in stores:
        copy.wait()
    sender.finish()


def default_order():
    order = []
    for step in range(13 + 2 * 2):
        for k in range(PIECES):
            phase = step - 2 * k
            if 0 <= phase < 13:
                order += [(UP, k), (DOWN, k), (MIXED, k)]
        if 1 <= step < 5:
            order.append("norm")
    return tuple(order)


ORDER = default_order()


def split_kernel(*refs):
    (
        copy_up, copy_down, copy_query, copy_key, copy_value, copy_mixed, kept, norm_out,
        o_copy_up, o_copy_down, o_copy_query, o_copy_key, o_copy_value, o_copy_mixed, o_copy_norm,
        o_new_up, o_new_down, o_new_query, o_new_key, o_new_value, o_new_mixed, o_new_norm,
        o_state_up, o_state_down, o_state_query, o_state_key, o_state_value, o_state_mixed, o_state_norm,
    ) = refs
    for source, target in (
        (copy_up, o_copy_up),
        (copy_down, o_copy_down),
        (copy_query, o_copy_query),
        (copy_key, o_copy_key),
        (copy_value, o_copy_value),
        (copy_mixed, o_copy_mixed),
    ):
        target[...] = source[...]
    o_copy_norm[...] = norm_out[0, 0:1].astype(jnp.bfloat16)
    for row, targets in enumerate(
        (
            (o_new_up, o_new_down, o_new_query, o_new_key, o_new_value, o_new_mixed),
            (o_state_up, o_state_down, o_state_query, o_state_key, o_state_value, o_state_mixed),
        )
    ):
        targets[0][...] = kept[row, UP]
        targets[1][...] = kept[row, DOWN]
        heads = kept[row, MIXED]
        for head in range(4):
            targets[2 + head][...] = heads[:, 192 * head : 192 * head + 192]
    o_new_norm[...] = norm_out[1, 0:1, 0:24]
    o_state_norm[...] = norm_out[1, 1:2, 0:24]


def on_device(
    grad_up, grad_down, grad_query, grad_key, grad_value, grad_mixed, grad_norm,
    weight_up, weight_down, weight_query, weight_key, weight_value, weight_mixed, weight_norm,
    moment_up, moment_down, moment_query, moment_key, moment_value, moment_mixed, moment_norm,
):
    f32, bf16 = jnp.float32, jnp.bfloat16
    anywhere = pl.BlockSpec(memory_space=pl.ANY)
    shape = jax.ShapeDtypeStruct
    operands = (
        grad_up[0].reshape(4, 4, 2, 24, 768), grad_down[0],
        grad_query[0].T, grad_key[0].T, grad_value[0].T, grad_mixed[0], grad_norm,
        weight_up, weight_down.T, weight_query, weight_key, weight_value, weight_mixed.T, weight_norm[None],
        moment_up, moment_down.T, moment_query, moment_key, moment_value, moment_mixed.T, moment_norm[None],
    )
    copy_shapes = (shape((768, 768), bf16),) * 2 + (shape((192, 768), bf16),) * 4
    gathered = pl.pallas_call(
        exchange_kernel,
        name="exchange",
        out_shape=copy_shapes + (shape((2, 3, 24, 768), f32), shape((2, 8, 768), f32)),
        in_specs=[anywhere] * 21,
        out_specs=[anywhere] * 8,
        scratch_shapes=[
            pltpu.VMEM((3, PIECES) + FOLDED, f32),
            pltpu.VMEM((2, 768, 768), f32),
            pltpu.VMEM((2, 3, 24, 768), f32),
            pltpu.VMEM((2, 4, 24, 192), f32),
            pltpu.VMEM((3, PIECES, 4, 4, 2, 48, HALF), bf16),
            pltpu.VMEM((3, 768, 768), bf16),
            pltpu.VMEM((2, 3, 24, 768), f32),
            pltpu.VMEM((2, 8, 768), f32),
            pltpu.VMEM((PIECES, 2, 2, 4, 24, WIDE), f32),
            pltpu.VMEM((PIECES, 2, 2, 4, 24, WIDE), f32),
            pltpu.VMEM((PIECES, 6, 2, 24, WIDE), f32),
            pltpu.VMEM((PIECES, 6, 24, HALF), f32),
            pltpu.VMEM((2, PIECES, 6, 2, 2, 24, WIDE), f32),
            pltpu.VMEM((2, PIECES, 6, 24, WIDE), f32),
            pltpu.VMEM((2, PIECES, 24, WIDE), f32),
            pltpu.VMEM((2, PIECES, 24, WIDE), f32),
            pltpu.VMEM((2, PIECES, 48, HALF), bf16),
            pltpu.VMEM((PIECES, 2, 2, 4, 48, HALF), bf16),
            pltpu.VMEM((1, 768), f32),
            pltpu.VMEM((2, 1, 24), f32),
            pltpu.VMEM((8, 768), f32),
            pltpu.VMEM((2, 8, 768), f32),
            pltpu.VMEM((2, 4, 8, 768), f32),
            pltpu.SemaphoreType.DMA((SENDS,)),
            pltpu.SemaphoreType.DMA((SENDS,)),
            pltpu.SemaphoreType.DMA((28,)),
            pltpu.SemaphoreType.DMA((12,)),
        ],
        compiler_params=pltpu.CompilerParams(collective_id=0, has_side_effects=True),
    )(*operands)
    kept_shapes = (
        (shape((24, 768), f32),) * 2 + (shape((24, 192), f32),) * 4 + (shape((1, 24), f32),)
    )
    outs = pl.pallas_call(
        split_kernel,
        name="split",
        out_shape=copy_shapes + (shape((1, 768), bf16),) + kept_shapes * 2,
    )(*gathered)
    copy_up, copy_down, copy_query, copy_key, copy_value, copy_mixed, copy_norm = outs[:7]

    def as_given(seven):
        up, down, query, key, value, mixed, norm = seven
        return (up, down.T, query, key, value, mixed.T, norm[0])

    return (
        (copy_up, copy_down, copy_query.T, copy_key.T, copy_value.T, copy_mixed, copy_norm[0])
        + as_given(outs[7:14])
        + as_given(outs[14:])
    )


def solution(mesh):
    return jax.shard_map(
        on_device,
        mesh=mesh,
        in_specs=(
            P("data", None, "width"),
            P("data", "width", None),
            P("data", None, "width"),
            P("data", None, "width"),
            P("data", None, "width"),
            P("data", "width", None),
            P("data", None),
        )
        + (
            P("data", "width"),
            P("width", "data"),
            P("data", "width"),
            P("data", "width"),
            P("data", "width"),
            P("width", "data"),
            P("data"),
        )
        * 2,
        out_specs=(
            P(None, "width"),
            P("width", None),
            P(None, "width"),
            P(None, "width"),
            P(None, "width"),
            P("width", None),
            P(),
        )
        + (
            P("data", "width"),
            P("width", "data"),
            P("data", "width"),
            P("data", "width"),
            P("data", "width"),
            P("width", "data"),
            P("data"),
        )
        * 2,
        check_vma=False,
    )
```

```python
import jax
import jax.numpy as jnp
from jax import lax
from jax.experimental import pallas as pl
from jax.experimental.pallas import tpu as pltpu
from jax.sharding import PartitionSpec as P

learn_rate = 0.05
hold_rate = 0.9
mean_rate = 32 ** (-0.5)

MESH = pl.DeviceIdType.MESH
WIDE = 256
HALF = 128
UP, DOWN, MIXED = 0, 1, 2
FOLDED = (4, 4, 2, 24, WIDE)
BLOCKS = 3
RAW = 6.0
SENDS = 196
STREAMS = (
    (UP, 0, 0, 24, "xyz", "dtd", "ddd"),
    (DOWN, 0, 0, 24, "zyx", "ttd", "tdd"),
    (MIXED, 0, 0, 24, "yzx", "ttd", "tdd"),
    (UP, 1, 0, 24, "xzy", "dtd", "ddd"),
    (DOWN, 1, 0, 24, "zyx", "ttd", "tdd"),
    (MIXED, 1, 0, 24, "yzx", "ttd", "tdd"),
    (UP, 2, 0, 24, "xyz", "dtd", "ddd"),
    (DOWN, 2, 0, 24, "zyx", "ttd", "tdd"),
    (MIXED, 2, 0, 24, "yzx", "ttd", "tdd"),
)
ORDER = (
    0, 1, 2, 3, 4, 5, 6, 7, 8, 9, 1, 2, 4, 5, 0, 7, 8, 1, 2, 4, 3, 5, 0, 7,
    2, 8, 1, 3, 4, 5, 6, 9, 0, 2, 7, 8, 1, 4, 3, 5, 6, 2, 0, 8, 9, 7, 1, 4,
    3, 5, 6, 2, 0, 9, 8, 7, 1, 4, 3, 5, 6, 8, 2, 7, 0, 1, 4, 3, 5, 2, 6, 8,
    7, 1, 5, 0, 4, 2, 7, 6, 3, 1, 8, 4, 7, 5, 8, 6,
)


def on_ring(step, size=4):
    return lax.rem(step, size)


class Place:
    def __init__(self):
        data, width = lax.axis_index("data"), lax.axis_index("width")
        self.z, self.y, self.xh = lax.div(data, 8), lax.rem(lax.div(data, 2), 4), lax.rem(data, 2)
        self.x, self.core = 2 * self.xh + lax.div(width, 2), lax.rem(width, 2)
        self.data = data

    def device(self, z, y, x):
        return (z * 8 + y * 2 + lax.div(x, 2), 2 * lax.rem(x, 2) + self.core)

    def along(self, axis, step):
        z, y, x = self.z, self.y, self.x
        if axis == "z":
            z = on_ring(z + step)
        elif axis == "y":
            y = on_ring(y + step)
        else:
            x = on_ring(x + step)
        return self.device(z, y, x)


class Sender:
    def __init__(self, place, send_sems, recv_sems):
        self.place, self.send_sems, self.recv_sems = place, send_sems, recv_sems
        self.copies = []

    def start(self, source, target, axis, step):
        n = len(self.copies)
        copy = pltpu.make_async_remote_copy(
            src_ref=source,
            dst_ref=target,
            send_sem=self.send_sems.at[n],
            recv_sem=self.recv_sems.at[n],
            device_id=self.place.along(axis, step),
            device_id_type=MESH,
        )
        copy.start()
        self.copies.append(copy)
        return copy

    def finish(self):
        for copy in self.copies:
            copy.wait_send()


def add_to(ref, *others):
    total = ref[...]
    for other in others:
        total = total + other[...]
    ref[...] = total


class Lines:
    def __init__(self, place, axes):
        self.at = {"z": place.z, "y": place.y, "x": place.xh}
        self.axes = axes

    def chosen(self, stage, q, half=None):
        index = dict(z=slice(None), y=slice(None), x=slice(None))
        for axis in self.axes[:stage]:
            index[axis] = self.at[axis]
        index[self.axes[stage]] = q
        if half is not None:
            split = self.axes[stage + 1] if self.axes[stage + 1] != "x" else self.axes[-1]
            index[split] = half if split == "x" else pl.ds(2 * half, 2)
        return index["z"], index["y"], index["x"]

    def span(self, stage, halved=False):
        sizes = dict(z=4, y=4, x=2)
        left = list(self.axes[stage + 1 :])
        shape = []
        split = None
        if halved:
            split = self.axes[stage + 1] if self.axes[stage + 1] != "x" else self.axes[-1]
        for axis in "zyx":
            if axis in left:
                if axis == split:
                    if axis != "x":
                        shape.append(2)
                else:
                    shape.append(sizes[axis])
        return tuple(shape)


def encode(values, largest):
    first = jnp.floor(values[:3] * ((2**18 - 1) / largest) + 0.5) * 64.0
    fourth = jnp.floor(values[3] * ((2**17 - 1) / largest) + (2**17 + 0.5))
    high = jnp.floor(fourth * 2.0**-12)
    rest = fourth - high * 4096.0
    middle = jnp.floor(rest * 2.0**-6)
    return first + jnp.stack([high, middle, rest - middle * 64.0])


def decode(coded, largest):
    first = jnp.floor(coded * 2.0**-6)
    digits = coded - first * 64.0
    fourth = (digits[0] * 64.0 + digits[1]) * 64.0 + (digits[2] - 2.0**17)
    return jnp.concatenate(
        [first * (largest / (2**18 - 1)), (fourth * (largest / (2**17 - 1)))[None]], axis=0
    )


def fours(ref):
    return ref[...].reshape((4,) + ref.shape[-2:])


def coded_stage(sender, lines, block, coded, landing):
    axis = lines.axes[0]
    at = lines.at[axis]
    if axis == "x":
        far = block(*lines.chosen(0, 1 - at))
        own = block(*lines.chosen(0, at))
        for n in range(4):
            coded[n] = encode(far[n], RAW)
        copy = sender.start(coded, landing, axis, 2)
        yield
        copy.wait_recv()
        for n in range(4):
            own[n] = own[n] + decode(landing[n], RAW)
        return
    plus, minus, opposite = on_ring(at + 1), on_ring(at + 3), on_ring(at + 2)

    def part(q, half):
        return block(*lines.chosen(0, q, half))

    def send(n, values, largest, step):
        coded[n] = encode(values, largest)
        return sender.start(coded.at[n], landing.at[n], axis, step)

    far_plus = send(0, fours(part(opposite, 0)), RAW, 1)
    far_minus = send(1, fours(part(opposite, 1)), RAW, 3)
    near_plus = send(2, fours(part(plus, 1)), RAW, 1)
    near_minus = send(3, fours(part(minus, 0)), RAW, 3)
    yield
    far_plus.wait_recv()
    both_plus = send(4, fours(part(plus, 0)) + decode(landing[0], RAW), 2 * RAW, 1)
    far_minus.wait_recv()
    both_minus = send(5, fours(part(minus, 1)) + decode(landing[1], RAW), 2 * RAW, 3)
    yield
    for near, near_slot, both, both_slot, half in (
        (near_minus, 3, both_plus, 4, 0),
        (near_plus, 2, both_minus, 5, 1),
    ):
        near.wait_recv()
        both.wait_recv()
        own = part(at, half)
        total = fours(own) + decode(landing[near_slot], RAW) + decode(landing[both_slot], 2 * RAW)
        own[...] = total.reshape(own.shape)


def scatter_stage(sender, lines, stage, mode, block, landing):
    axis = lines.axes[stage]
    at = lines.at[axis]
    own = block(*lines.chosen(stage, at))
    if axis == "x":
        copy = sender.start(block(*lines.chosen(stage, 1 - at)), landing.at[0], axis, 2)
        yield
        copy.wait_recv()
        add_to(own, landing.at[0])
        return
    plus, minus, opposite = on_ring(at + 1), on_ring(at + 3), on_ring(at + 2)
    if mode == "d":
        copies = [
            sender.start(block(*lines.chosen(stage, q)), landing.at[n], axis, step)
            for n, (q, step) in enumerate(((opposite, 2), (plus, 1), (minus, 3)))
        ]
        yield
        for copy in copies:
            copy.wait_recv()
        add_to(own, *(landing.at[n] for n in range(3)))
        return

    def part(q, half):
        return block(*lines.chosen(stage, q, half))

    far_plus = sender.start(part(opposite, 0), landing.at[0], axis, 1)
    far_minus = sender.start(part(opposite, 1), landing.at[1], axis, 3)
    near_plus = sender.start(part(plus, 1), landing.at[2], axis, 1)
    near_minus = sender.start(part(minus, 0), landing.at[3], axis, 3)
    yield
    far_plus.wait_recv()
    add_to(part(plus, 0), landing.at[0])
    both_plus = sender.start(part(plus, 0), landing.at[4], axis, 1)
    far_minus.wait_recv()
    add_to(part(minus, 1), landing.at[1])
    both_minus = sender.start(part(minus, 1), landing.at[5], axis, 3)
    yield
    near_minus.wait_recv()
    both_plus.wait_recv()
    add_to(part(at, 0), landing.at[3], landing.at[4])
    near_plus.wait_recv()
    both_minus.wait_recv()
    add_to(part(at, 1), landing.at[2], landing.at[5])


def gather_stage(sender, lines, stage, mode, block):
    axis = lines.axes[stage]
    at = lines.at[axis]
    own = block(*lines.chosen(stage, at))
    if axis == "x" or mode == "d":
        copies = [sender.start(own, own, axis, step) for step in ((2,) if axis == "x" else (2, 1, 3))]
        yield
        for copy in copies:
            copy.wait_recv()
        return

    def part(q, half):
        return block(*lines.chosen(stage, q, half))

    plus, minus = on_ring(at + 1), on_ring(at + 3)
    first_plus = sender.start(part(at, 0), part(at, 0), axis, 1)
    first_minus = sender.start(part(at, 1), part(at, 1), axis, 3)
    second_plus = sender.start(part(at, 1), part(at, 1), axis, 1)
    second_minus = sender.start(part(at, 0), part(at, 0), axis, 3)
    yield
    first_plus.wait_recv()
    on_plus = sender.start(part(minus, 0), part(minus, 0), axis, 1)
    first_minus.wait_recv()
    on_minus = sender.start(part(plus, 1), part(plus, 1), axis, 3)
    yield
    for copy in (second_plus, second_minus, on_plus, on_minus):
        copy.wait_recv()


def updated(mean, weight, moment):
    state = hold_rate * moment + (1.0 - hold_rate) * mean * mean
    return weight - learn_rate * mean * lax.rsqrt(state + 1e-06), state


def exchange_kernel(*refs):
    (
        grad_up, grad_down, grad_query, grad_key, grad_value, grad_mixed, grad_norm,
        weight_up, weight_down, weight_query, weight_key, weight_value, weight_mixed, weight_norm,
        moment_up, moment_down, moment_query, moment_key, moment_value, moment_mixed, moment_norm,
        out_up, out_down, out_mixed, norm_all,
        new_up, new_down, new_query, new_key, new_value, new_mixed, new_norm,
        state_up, state_down, state_query, state_key, state_value, state_mixed, state_norm,
        sums, turned, held, held_heads, whole, mixed_own,
        norm_grad, norm_held, norm_rows, norm_pair, norm_ring,
        send_sems, recv_sems, load_sems,
        *landings,
    ) = refs
    place = Place()
    z, y, xh = place.z, place.y, place.xh
    columns = [pl.ds(WIDE * k, WIDE) for k in range(BLOCKS)]

    barrier = pltpu.get_barrier_semaphore()
    for axis in ("x", "y", "z"):
        for step in (2,) if axis == "x" else (1, 2, 3):
            pl.semaphore_signal(barrier, inc=1, device_id=place.along(axis, step), device_id_type=MESH)

    loads = {}

    def load(name, source, target):
        copy = pltpu.make_async_copy(source, target, load_sems.at[len(loads)])
        copy.start()
        loads[name] = copy

    heads = (grad_query, grad_key, grad_value, grad_mixed)
    for k in range(BLOCKS):
        load((UP, k), grad_up.at[:, :, :, :, columns[k]], sums.at[UP, k])
        load((DOWN, k), grad_down.at[columns[k], :], turned.at[0, columns[k], :])
        for head in ((0, 1), (2,), (3,))[k]:
            load(("head", head), heads[head], turned.at[1, pl.ds(192 * head, 192), :])
    load("norm", grad_norm, norm_grad)
    load("weight_norm", weight_norm, norm_held.at[0])
    load("moment_norm", moment_norm, norm_held.at[1])
    load(("weight", UP), weight_up, held.at[0, UP])
    load(("moment", UP), moment_up, held.at[1, UP])
    load(("weight", DOWN), weight_down, held.at[0, DOWN])
    load(("moment", DOWN), moment_down, held.at[1, DOWN])
    for head, source in enumerate((weight_query, weight_key, weight_value, weight_mixed)):
        load(("weight head", head), source, held_heads.at[0, head])
    for head, source in enumerate((moment_query, moment_key, moment_value, moment_mixed)):
        load(("moment head", head), source, held_heads.at[1, head])

    sender = Sender(place, send_sems, recv_sems)
    gathered = {}
    ready = set()

    def make_ready(part, k):
        if (part, k) in ready:
            return
        ready.add((part, k))
        if part == UP:
            loads[UP, k].wait()
            return
        if part == DOWN:
            loads[DOWN, k].wait()
        else:
            for head in ((0, 1), (2,), (3,))[k]:
                loads["head", head].wait()

        def turn(n, carry):
            lanes = pl.ds(pl.multiple_of(384 * n, HALF), 384)
            tile = turned[part - 1, columns[k], lanes]
            sums[part, k, pl.ds(2 * n, 2)] = tile.T.reshape(2, 4, 2, 24, WIDE)
            return carry

        lax.fori_loop(0, 2, turn, 0)

    def hold(part):
        if ("held", part) in ready:
            return
        ready.add(("held", part))
        if part != MIXED:
            loads["weight", part].wait()
            loads["moment", part].wait()
            return
        for row, name in enumerate(("weight head", "moment head")):
            for head in range(4):
                loads[name, head].wait()
            held[row, part] = jnp.concatenate([held_heads[row, head] for head in range(4)], axis=1)

    def finish(part, k, rows):
        done = gathered.setdefault((part, k), [])
        done.append(rows)
        if sum(count for _, count in done) < 24:
            return
        done.sort()

        def side(chunk, half):
            return [
                chunk[..., 2 * first + count * half : 2 * first + count * half + count, :]
                for first, count in done
            ]

        if part == UP:

            def pair_of_chunks(n, carry):
                chunks = [
                    whole[UP, k, lax.div(n, 4), lax.rem(n, 4), c].astype(jnp.float32) for c in range(2)
                ]
                at = pl.ds(pl.multiple_of(48 * n, 16), 48)
                for half in range(2):
                    both = jnp.concatenate(side(chunks[0], half) + side(chunks[1], half), axis=0)
                    out_up[at, pl.ds(WIDE * k + HALF * half, HALF)] = both.astype(jnp.bfloat16)
                return carry

            lax.fori_loop(0, 16, pair_of_chunks, 0)
            return
        for half in range(2):
            chunks = whole[part, k].astype(jnp.float32)
            tile = jnp.concatenate(side(chunks, half), axis=-2)
            (out_down, out_mixed)[part - 1][pl.ds(WIDE * k + HALF * half, HALF), :] = (
                tile.reshape(768, HALF).T.astype(jnp.bfloat16)
            )

    def keep(part, k, rows, new, state):
        if part != MIXED:
            (new_up, new_down)[part][rows, columns[k]] = new
            (state_up, state_down)[part][rows, columns[k]] = state
            return
        mixed_own[0, rows, columns[k]] = new
        mixed_own[1, rows, columns[k]] = state
        gathered["kept"] = gathered.get("kept", 0) + 1
        if gathered["kept"] == sum(piece[0] == MIXED for piece in STREAMS):
            for row, targets in enumerate(
                ((new_query, new_key, new_value, new_mixed), (state_query, state_key, state_value, state_mixed))
            ):
                everything = mixed_own[row]
                for head in range(4):
                    targets[head][...] = everything[:, 192 * head : 192 * head + 192]

    def stream(part, k, first, count, axes, scatter_modes, gather_modes, lands):
        rows = pl.ds(first, count)
        copied = pl.ds(2 * first, 2 * count)
        lines = Lines(place, axes)

        def block(*index):
            return sums.at[(part, k) + index + (rows, slice(None))]

        def copy_block(*index):
            return whole.at[(part, k) + index + (copied, slice(None))]

        make_ready(part, k)
        coded, *lands = lands
        yield from coded_stage(sender, lines, block, coded, lands[0])
        for stage in (1, 2):
            yield from scatter_stage(sender, lines, stage, scatter_modes[stage], block, lands[stage])
        hold(part)
        own = sums[part, k, z, y, xh, rows, :] * mean_rate
        new, state = updated(own, held[0, part, rows, columns[k]], held[1, part, rows, columns[k]])
        keep(part, k, rows, new, state)
        whole[part, k, z, y, xh, copied, :] = jnp.concatenate(
            [new[:, :HALF], new[:, HALF:]], axis=0
        ).astype(jnp.bfloat16)
        for stage in (2, 1, 0):
            yield from gather_stage(sender, lines, stage, gather_modes[stage], copy_block)
        finish(part, k, (first, count))

    def norm_stream():
        for name in ("norm", "weight_norm", "moment_norm"):
            loads[name].wait()
        norm_rows[...] = jnp.zeros_like(norm_rows)
        norm_rows[1:2, 0:24] = norm_held[0]
        norm_rows[2:3, 0:24] = norm_held[1]
        placed = pltpu.roll(norm_rows[...], 24 * place.data, 1)
        norm_pair[xh, 0] = norm_grad[...]
        norm_pair[xh, 1] = placed[1:2]
        norm_pair[xh, 2] = placed[2:3]
        copy = sender.start(norm_pair.at[xh], norm_pair.at[xh], "x", 2)
        yield
        copy.wait_recv()
        norm_ring[0, y] = norm_pair[0] + norm_pair[1]
        copies = [sender.start(norm_ring.at[0, y], norm_ring.at[0, y], "y", s) for s in (1, 2, 3)]
        yield
        for copy in copies:
            copy.wait_recv()
        norm_ring[1, z] = norm_ring[0, 0] + norm_ring[0, 1] + norm_ring[0, 2] + norm_ring[0, 3]
        copies = [sender.start(norm_ring.at[1, z], norm_ring.at[1, z], "z", s) for s in (1, 2, 3)]
        yield
        for copy in copies:
            copy.wait_recv()
        total = norm_ring[1, 0] + norm_ring[1, 1] + norm_ring[1, 2] + norm_ring[1, 3]
        new, state = updated(total[0] * mean_rate, total[1], total[2])
        norm_all[...] = new
        norm_rows[0:1] = new
        norm_rows[1:2] = state
        own = pltpu.roll(norm_rows[...], lax.rem(768 - 24 * place.data, 768), 1)
        new_norm[...] = own[0:1, 0:24]
        state_norm[...] = own[1:2, 0:24]

    streams = []
    for n, piece in enumerate(STREAMS):
        streams.append(stream(*piece, landings[4 * n : 4 * n + 4]))
    streams.append(norm_stream())
    for part in (UP, DOWN, MIXED):
        make_ready(part, 0)
    pl.semaphore_wait(barrier, 7)
    for n in ORDER:
        next(streams[n], None)
    sender.finish()


def landing_shapes():
    shapes = []
    for part, k, first, count, axes, scatter_modes, gather_modes in STREAMS:
        lines = Lines.__new__(Lines)
        lines.axes = axes
        first_shape = (4 if axes[0] == "x" else 6, 3, count, WIDE)
        shapes += [pltpu.VMEM(first_shape, jnp.float32)] * 2
        for stage in (1, 2):
            twice = axes[stage] != "x" and scatter_modes[stage] == "t"
            slots = 1 if axes[stage] == "x" else 6 if twice else 3
            shapes.append(pltpu.VMEM((slots,) + lines.span(stage, twice) + (count, WIDE), jnp.float32))
    return shapes


def split_kernel(up, down, mixed, norm_all, *rest):
    kept, (copy_up, copy_down, *heads, copy_norm), others, sems = rest[:14], rest[14:21], rest[21:35], rest[35]
    pairs = [(up, copy_up), (down, copy_down)]
    pairs += [(mixed.at[pl.ds(192 * n, 192), :], head) for n, head in enumerate(heads)]
    pairs += list(zip(kept, others))
    copies = [pltpu.make_async_copy(source, target, sems.at[n]) for n, (source, target) in enumerate(pairs)]
    for copy in copies:
        copy.start()
    copy_norm[...] = norm_all[0].astype(jnp.bfloat16)
    for copy in copies:
        copy.wait()


def on_device(
    grad_up, grad_down, grad_query, grad_key, grad_value, grad_mixed, grad_norm,
    weight_up, weight_down, weight_query, weight_key, weight_value, weight_mixed, weight_norm,
    moment_up, moment_down, moment_query, moment_key, moment_value, moment_mixed, moment_norm,
):
    f32, bf16 = jnp.float32, jnp.bfloat16
    anywhere = pl.BlockSpec(memory_space=pl.ANY)
    shape = jax.ShapeDtypeStruct
    operands = (
        grad_up[0].reshape(4, 4, 2, 24, 768), grad_down[0],
        grad_query[0].T, grad_key[0].T, grad_value[0].T, grad_mixed[0], grad_norm,
        weight_up, weight_down.T, weight_query, weight_key, weight_value, weight_mixed.T, weight_norm[None],
        moment_up, moment_down.T, moment_query, moment_key, moment_value, moment_mixed.T, moment_norm[None],
    )
    vmem = pl.BlockSpec(memory_space=pltpu.VMEM)
    kept_shapes = ((24, 768),) * 2 + ((24, 192),) * 4 + ((1, 24),)
    inner = (pltpu.VMEM((768, 768), bf16),) * 3 + (pltpu.VMEM((1, 768), f32),)
    inner += tuple(pltpu.VMEM(s, f32) for s in kept_shapes * 2)
    results = pl.pallas_call(
        exchange_kernel,
        name="exchange",
        out_shape=inner,
        in_specs=[anywhere] * 21,
        out_specs=[vmem] * 18,
        scratch_shapes=[
            pltpu.VMEM((3, BLOCKS) + FOLDED, f32),
            pltpu.VMEM((2, 768, 768), f32),
            pltpu.VMEM((2, 3, 24, 768), f32),
            pltpu.VMEM((2, 4, 24, 192), f32),
            pltpu.VMEM((3, BLOCKS, 4, 4, 2, 48, HALF), bf16),
            pltpu.VMEM((2, 24, 768), f32),
            pltpu.VMEM((1, 768), f32),
            pltpu.VMEM((2, 1, 24), f32),
            pltpu.VMEM((8, 768), f32),
            pltpu.VMEM((2, 3, 1, 768), f32),
            pltpu.VMEM((2, 4, 3, 1, 768), f32),
            pltpu.SemaphoreType.DMA((SENDS,)),
            pltpu.SemaphoreType.DMA((SENDS,)),
            pltpu.SemaphoreType.DMA((28,)),
        ]
        + landing_shapes(),
        compiler_params=pltpu.CompilerParams(
            collective_id=0, has_side_effects=True, vmem_limit_bytes=56 * 2**20
        ),
    )(*operands)
    outs = pl.pallas_call(
        split_kernel,
        name="split",
        out_shape=(shape((768, 768), bf16),) * 2
        + (shape((192, 768), bf16),) * 4
        + (shape((768,), bf16),)
        + tuple(shape(s, f32) for s in kept_shapes * 2),
        in_specs=[vmem] * 18,
        out_specs=[anywhere] * 6 + [vmem] + [anywhere] * 14,
        scratch_shapes=[pltpu.SemaphoreType.DMA((20,))],
        compiler_params=pltpu.CompilerParams(vmem_limit_bytes=8 * 2**20),
    )(*results)
    copy_up, copy_down, copy_query, copy_key, copy_value, copy_mixed, copy_norm = outs[:7]

    def as_given(seven):
        up, down, query, key, value, mixed, norm = seven
        return (up, down.T, query, key, value, mixed.T, norm[0])

    return (
        (copy_up, copy_down, copy_query.T, copy_key.T, copy_value.T, copy_mixed, copy_norm)
        + as_given(outs[7:14])
        + as_given(outs[14:])
    )


def solution(mesh):
    return jax.shard_map(
        on_device,
        mesh=mesh,
        in_specs=(
            P("data", None, "width"),
            P("data", "width", None),
            P("data", None, "width"),
            P("data", None, "width"),
            P("data", None, "width"),
            P("data", "width", None),
            P("data", None),
        )
        + (
            P("data", "width"),
            P("width", "data"),
            P("data", "width"),
            P("data", "width"),
            P("data", "width"),
            P("width", "data"),
            P("data"),
        )
        * 2,
        out_specs=(
            P(None, "width"),
            P("width", None),
            P(None, "width"),
            P(None, "width"),
            P(None, "width"),
            P("width", None),
            P(),
        )
        + (
            P("data", "width"),
            P("width", "data"),
            P("data", "width"),
            P("data", "width"),
            P("data", "width"),
            P("width", "data"),
            P("data"),
        )
        * 2,
        check_vma=False,
    )
```

```python
import jax
import jax.numpy as jnp
from jax import lax
from jax.experimental import pallas as pl
from jax.experimental.pallas import tpu as pltpu
from jax.sharding import PartitionSpec as P

learn_rate = 0.05
hold_rate = 0.9
mean_rate = 32 ** (-0.5)

MESH = pl.DeviceIdType.MESH
WIDE = 256
HALF = 128
UP, DOWN, MIXED = 0, 1, 2
FOLDED = (4, 4, 2, 24, WIDE)
BLOCKS = 3
RAW = 6.0
STREAMS = (
    (UP, 0, 0, 24, "xyz", "dtd", "ddd"),
    (DOWN, 0, 0, 24, "yxz", "tdd", "tdd"),
    (MIXED, 0, 0, 24, "zxy", "tdd", "tdd"),
    (UP, 1, 0, 24, "xzy", "dtd", "ddd"),
    (DOWN, 1, 0, 24, "zyx", "ttd", "tdd"),
    (MIXED, 1, 0, 24, "yxz", "tdd", "tdd"),
    (UP, 2, 0, 16, "yxz", "tdd", "tdd"),
    (DOWN, 2, 0, 16, "zyx", "ttd", "tdd"),
    (MIXED, 2, 0, 16, "yzx", "tdd", "tdd"),
    (UP, 2, 16, 8, "zxy", "tdd", "tdd"),
    (DOWN, 2, 16, 8, "zxy", "tdd", "tdd"),
    (MIXED, 2, 16, 8, "xzy", "ddd", "ddd"),
)
ORDER = (
    0, 1, 2, 3, 4, 5, 6, 7, 8, 9, 10, 11, 12, 1, 2, 5, 4, 0, 6, 7, 9, 8, 10, 1,
    2, 3, 5, 4, 0, 11, 7, 12, 9, 10, 6, 3, 1, 8, 4, 11, 2, 0, 7, 3, 12, 5, 4, 1,
    9, 11, 10, 8, 2, 7, 6, 0, 12, 3, 4, 9, 5, 1, 10, 8, 11, 2, 7, 6, 0, 3, 4, 9,
    5, 10, 1, 11, 8, 6, 2, 7, 9, 0, 3, 5, 10, 4, 8, 1, 11, 2, 6, 7, 9, 10, 5, 4,
    8, 0, 2, 1, 7, 6, 9, 10, 5, 4, 8, 3, 7, 6,
)


def on_ring(step, size=4):
    return lax.rem(step, size)


class Place:
    def __init__(self):
        data, width = lax.axis_index("data"), lax.axis_index("width")
        self.z, self.y, self.xh = lax.div(data, 8), lax.rem(lax.div(data, 2), 4), lax.rem(data, 2)
        self.x, self.core = 2 * self.xh + lax.div(width, 2), lax.rem(width, 2)
        self.data = data

    def device(self, z, y, x):
        return (z * 8 + y * 2 + lax.div(x, 2), 2 * lax.rem(x, 2) + self.core)

    def along(self, axis, step):
        z, y, x = self.z, self.y, self.x
        if axis == "z":
            z = on_ring(z + step)
        elif axis == "y":
            y = on_ring(y + step)
        else:
            x = on_ring(x + step)
        return self.device(z, y, x)


class Sender:
    def __init__(self, place, send_sems, recv_sems, first):
        self.place, self.send_sems, self.recv_sems = place, send_sems, recv_sems
        self.next_send, self.next_recv = first
        self.sent = []
        self.turn = 0

    def landing(self):
        self.next_recv += 1
        return self.recv_sems.at[self.next_recv - 1]

    def begin(self, size):
        sem = self.send_sems.at[self.next_send + self.turn]
        self.turn = 1 - self.turn
        if len(self.sent) == 2:
            wait_for(*self.sent.pop(0))
        self.sent.append((size, sem))

    def start(self, source, target, axis, step, landing):
        pltpu.make_async_remote_copy(
            src_ref=source,
            dst_ref=target,
            send_sem=self.sent[-1][1],
            recv_sem=landing,
            device_id=self.place.along(axis, step),
            device_id_type=MESH,
        ).start()

    def finish(self):
        for size, sem in self.sent:
            wait_for(size, sem)


def wait_for(size, sem):
    pltpu.make_async_copy(size, size, sem).wait()


def add_to(ref, *others):
    total = ref[...]
    for other in others:
        total = total + other[...]
    ref[...] = total


class Lines:
    def __init__(self, place, axes):
        self.at = {"z": place.z, "y": place.y, "x": place.xh}
        self.axes = axes

    def chosen(self, stage, q, half=None):
        index = dict(z=slice(None), y=slice(None), x=slice(None))
        for axis in self.axes[:stage]:
            index[axis] = self.at[axis]
        index[self.axes[stage]] = q
        if half is not None:
            split = self.axes[stage + 1] if self.axes[stage + 1] != "x" else self.axes[-1]
            index[split] = half if split == "x" else pl.ds(2 * half, 2)
        return index["z"], index["y"], index["x"]

    def span(self, stage, halved=False):
        sizes = dict(z=4, y=4, x=2)
        left = list(self.axes[stage + 1 :])
        shape = []
        split = None
        if halved:
            split = self.axes[stage + 1] if self.axes[stage + 1] != "x" else self.axes[-1]
        for axis in "zyx":
            if axis in left:
                if axis == split:
                    if axis != "x":
                        shape.append(2)
                else:
                    shape.append(sizes[axis])
        return tuple(shape)


def encode(values, largest):
    first = jnp.floor(values[:3] * ((2**18 - 1) / largest) + 0.5) * 64.0
    fourth = jnp.floor(values[3] * ((2**17 - 1) / largest) + (2**17 + 0.5))
    high = jnp.floor(fourth * 2.0**-12)
    rest = fourth - high * 4096.0
    middle = jnp.floor(rest * 2.0**-6)
    return first + jnp.stack([high, middle, rest - middle * 64.0])


def decode(coded, largest):
    first = jnp.floor(coded * 2.0**-6)
    digits = coded - first * 64.0
    fourth = (digits[0] * 64.0 + digits[1]) * 64.0 + (digits[2] - 2.0**17)
    return jnp.concatenate(
        [first * (largest / (2**18 - 1)), (fourth * (largest / (2**17 - 1)))[None]], axis=0
    )


def fours(ref):
    return ref[...].reshape((4,) + ref.shape[-2:])


def coded_stage(sender, lines, block, coded, landing):
    axis = lines.axes[0]
    at = lines.at[axis]
    if axis == "x":
        far = block(*lines.chosen(0, 1 - at))
        own = block(*lines.chosen(0, at))
        for n in range(4):
            coded[n] = encode(far[n], RAW)
        arrived = sender.landing()
        sender.begin(landing)
        sender.start(coded, landing, axis, 2, arrived)
        yield
        wait_for(landing, arrived)
        for n in range(4):
            own[n] = own[n] + decode(landing[n], RAW)
        return
    plus, minus, opposite = on_ring(at + 1), on_ring(at + 3), on_ring(at + 2)

    def part(q, half):
        return block(*lines.chosen(0, q, half))

    far, final = sender.landing(), sender.landing()

    def send(n, values, largest, step, arrived):
        coded[n] = encode(values, largest)
        sender.start(coded.at[n], landing.at[n], axis, step, arrived)

    sender.begin(landing.at[0:4])
    send(0, fours(part(opposite, 0)), RAW, 1, far)
    send(1, fours(part(opposite, 1)), RAW, 3, far)
    send(2, fours(part(plus, 1)), RAW, 1, final)
    send(3, fours(part(minus, 0)), RAW, 3, final)
    yield
    wait_for(landing.at[0:2], far)
    sender.begin(landing.at[4:6])
    send(4, fours(part(plus, 0)) + decode(landing[0], RAW), 2 * RAW, 1, final)
    send(5, fours(part(minus, 1)) + decode(landing[1], RAW), 2 * RAW, 3, final)
    yield
    wait_for(landing.at[2:6], final)
    for near, both, half in ((3, 4, 0), (2, 5, 1)):
        own = part(at, half)
        total = fours(own) + decode(landing[near], RAW) + decode(landing[both], 2 * RAW)
        own[...] = total.reshape(own.shape)


def scatter_stage(sender, lines, stage, mode, block, landing):
    axis = lines.axes[stage]
    at = lines.at[axis]
    own = block(*lines.chosen(stage, at))
    plus, minus, opposite = on_ring(at + 1), on_ring(at + 3), on_ring(at + 2)
    if axis == "x" or mode == "d":
        arrived = sender.landing()
        sender.begin(landing)
        targets = ((1 - at, 2),) if axis == "x" else ((opposite, 2), (plus, 1), (minus, 3))
        for n, (q, step) in enumerate(targets):
            sender.start(block(*lines.chosen(stage, q)), landing.at[n], axis, step, arrived)
        yield
        wait_for(landing, arrived)
        add_to(own, *(landing.at[n] for n in range(len(targets))))
        return

    def part(q, half):
        return block(*lines.chosen(stage, q, half))

    far, final = sender.landing(), sender.landing()
    sender.begin(landing.at[0:4])
    sender.start(part(opposite, 0), landing.at[0], axis, 1, far)
    sender.start(part(opposite, 1), landing.at[1], axis, 3, far)
    sender.start(part(plus, 1), landing.at[2], axis, 1, final)
    sender.start(part(minus, 0), landing.at[3], axis, 3, final)
    yield
    wait_for(landing.at[0:2], far)
    sender.begin(landing.at[4:6])
    add_to(part(plus, 0), landing.at[0])
    sender.start(part(plus, 0), landing.at[4], axis, 1, final)
    add_to(part(minus, 1), landing.at[1])
    sender.start(part(minus, 1), landing.at[5], axis, 3, final)
    yield
    wait_for(landing.at[2:6], final)
    add_to(part(at, 0), landing.at[3], landing.at[4])
    add_to(part(at, 1), landing.at[2], landing.at[5])


def gather_stage(sender, lines, stage, mode, block):
    axis = lines.axes[stage]
    at = lines.at[axis]
    own = block(*lines.chosen(stage, at))
    if axis == "x" or mode == "d":
        steps = (2,) if axis == "x" else (2, 1, 3)
        arrived = sender.landing()
        size = block(*lines.chosen(stage, pl.ds(0, len(steps))))
        sender.begin(size)
        for step in steps:
            sender.start(own, own, axis, step, arrived)
        yield
        wait_for(size, arrived)
        return

    def part(q, half):
        return block(*lines.chosen(stage, q, half))

    plus, minus = on_ring(at + 1), on_ring(at + 3)
    near, final = sender.landing(), sender.landing()
    two = block(*lines.chosen(stage, pl.ds(0, 2)))
    sender.begin(two)
    sender.start(part(at, 0), part(at, 0), axis, 1, near)
    sender.start(part(at, 1), part(at, 1), axis, 3, near)
    sender.start(part(at, 1), part(at, 1), axis, 1, final)
    sender.start(part(at, 0), part(at, 0), axis, 3, final)
    yield
    wait_for(own, near)
    sender.begin(own)
    sender.start(part(minus, 0), part(minus, 0), axis, 1, final)
    sender.start(part(plus, 1), part(plus, 1), axis, 3, final)
    yield
    wait_for(two, final)


def updated(mean, weight, moment):
    state = hold_rate * moment + (1.0 - hold_rate) * mean * mean
    return weight - learn_rate * mean * lax.rsqrt(state + 1e-06), state


def exchange_kernel(*refs):
    (
        grad_up, grad_down, grad_query, grad_key, grad_value, grad_mixed, grad_norm,
        weight_up, weight_down, weight_query, weight_key, weight_value, weight_mixed, weight_norm,
        moment_up, moment_down, moment_query, moment_key, moment_value, moment_mixed, moment_norm,
        out_up, out_down, out_mixed, norm_all,
        new_up, new_down, new_query, new_key, new_value, new_mixed, new_norm,
        state_up, state_down, state_query, state_key, state_value, state_mixed, state_norm,
        sums, turned, held, held_heads, whole, mixed_own,
        norm_grad, norm_held, norm_rows, norm_pair, norm_ring,
        send_sems, recv_sems, load_sems,
        *landings,
    ) = refs
    place = Place()
    z, y, xh = place.z, place.y, place.xh
    columns = [pl.ds(WIDE * k, WIDE) for k in range(BLOCKS)]

    barrier = pltpu.get_barrier_semaphore()
    for axis in ("x", "y", "z"):
        for step in (2,) if axis == "x" else (1, 2, 3):
            pl.semaphore_signal(barrier, inc=1, device_id=place.along(axis, step), device_id_type=MESH)

    loads = {}

    def load(name, *pairs, size=None):
        sem = load_sems.at[len(loads)]
        for source, target in pairs:
            pltpu.make_async_copy(source, target, sem).start()
        loads[name] = pairs[0][1] if size is None else size, sem

    def loaded(name):
        wait_for(*loads[name])

    heads = (grad_query, grad_key, grad_value, grad_mixed)
    for k in range(BLOCKS):
        load((UP, k), (grad_up.at[:, :, :, :, columns[k]], sums.at[UP, k]))
        load((DOWN, k), (grad_down.at[columns[k], :], turned.at[0, columns[k], :]))
        for head in ((0, 1), (2,), (3,))[k]:
            load(("head", head), (heads[head], turned.at[1, pl.ds(192 * head, 192), :]))
    load("norm", (grad_norm, norm_grad))
    load("held norm", (weight_norm, norm_held.at[0]), (moment_norm, norm_held.at[1]), size=norm_held)
    for part, weight, moment in ((UP, weight_up, moment_up), (DOWN, weight_down, moment_down)):
        load(
            ("held", part), (weight, held.at[0, part]), (moment, held.at[1, part]), size=held.at[:, part]
        )
    four_weights = (weight_query, weight_key, weight_value, weight_mixed)
    four_moments = (moment_query, moment_key, moment_value, moment_mixed)
    load(
        ("held", MIXED),
        *((source, held_heads.at[0, head]) for head, source in enumerate(four_weights)),
        *((source, held_heads.at[1, head]) for head, source in enumerate(four_moments)),
        size=held_heads,
    )

    gathered = {}
    ready = set()

    def make_ready(part, k):
        if (part, k) in ready:
            return
        ready.add((part, k))
        if part == UP:
            loaded((UP, k))
            return
        if part == DOWN:
            loaded((DOWN, k))
        else:
            for head in ((0, 1), (2,), (3,))[k]:
                loaded(("head", head))

        def turn(n, carry):
            lanes = pl.ds(pl.multiple_of(384 * n, HALF), 384)
            tile = turned[part - 1, columns[k], lanes]
            sums[part, k, pl.ds(2 * n, 2)] = tile.T.reshape(2, 4, 2, 24, WIDE)
            return carry

        lax.fori_loop(0, 2, turn, 0)

    def hold(part):
        if ("held", part) in ready:
            return
        ready.add(("held", part))
        loaded(("held", part))
        if part == MIXED:
            for row in range(2):
                held[row, part] = jnp.concatenate([held_heads[row, head] for head in range(4)], axis=1)

    def finish(part, k, rows):
        done = gathered.setdefault((part, k), [])
        done.append(rows)
        if sum(count for _, count in done) < 24:
            return
        done.sort()

        def side(chunk, half):
            return [
                chunk[..., 2 * first + count * half : 2 * first + count * half + count, :]
                for first, count in done
            ]

        if part == UP:

            def pair_of_chunks(n, carry):
                chunks = [
                    whole[UP, k, lax.div(n, 4), lax.rem(n, 4), c].astype(jnp.float32) for c in range(2)
                ]
                at = pl.ds(pl.multiple_of(48 * n, 16), 48)
                for half in range(2):
                    both = jnp.concatenate(side(chunks[0], half) + side(chunks[1], half), axis=0)
                    out_up[at, pl.ds(WIDE * k + HALF * half, HALF)] = both.astype(jnp.bfloat16)
                return carry

            lax.fori_loop(0, 16, pair_of_chunks, 0)
            return
        for half in range(2):
            chunks = whole[part, k].astype(jnp.float32)
            tile = jnp.concatenate(side(chunks, half), axis=-2)
            (out_down, out_mixed)[part - 1][pl.ds(WIDE * k + HALF * half, HALF), :] = (
                tile.reshape(768, HALF).T.astype(jnp.bfloat16)
            )

    def keep(part, k, rows, new, state):
        if part != MIXED:
            (new_up, new_down)[part][rows, columns[k]] = new
            (state_up, state_down)[part][rows, columns[k]] = state
            return
        mixed_own[0, rows, columns[k]] = new
        mixed_own[1, rows, columns[k]] = state
        gathered["kept"] = gathered.get("kept", 0) + 1
        if gathered["kept"] == sum(piece[0] == MIXED for piece in STREAMS):
            for row, targets in enumerate(
                ((new_query, new_key, new_value, new_mixed), (state_query, state_key, state_value, state_mixed))
            ):
                everything = mixed_own[row]
                for head in range(4):
                    targets[head][...] = everything[:, 192 * head : 192 * head + 192]

    def stream(sender, part, k, first, count, axes, scatter_modes, gather_modes, lands):
        rows = pl.ds(first, count)
        copied = pl.ds(2 * first, 2 * count)
        lines = Lines(place, axes)

        def block(*index):
            return sums.at[(part, k) + index + (rows, slice(None))]

        def copy_block(*index):
            return whole.at[(part, k) + index + (copied, slice(None))]

        make_ready(part, k)
        coded, *lands = lands
        yield from coded_stage(sender, lines, block, coded, lands[0])
        for stage in (1, 2):
            yield from scatter_stage(sender, lines, stage, scatter_modes[stage], block, lands[stage])
        hold(part)
        own = sums[part, k, z, y, xh, rows, :] * mean_rate
        new, state = updated(own, held[0, part, rows, columns[k]], held[1, part, rows, columns[k]])
        keep(part, k, rows, new, state)
        whole[part, k, z, y, xh, copied, :] = jnp.concatenate(
            [new[:, :HALF], new[:, HALF:]], axis=0
        ).astype(jnp.bfloat16)
        for stage in (2, 1, 0):
            yield from gather_stage(sender, lines, stage, gather_modes[stage], copy_block)
        finish(part, k, (first, count))

    def norm_stream(sender):
        loaded("norm")
        loaded("held norm")
        norm_rows[...] = jnp.zeros_like(norm_rows)
        norm_rows[1:2, 0:24] = norm_held[0]
        norm_rows[2:3, 0:24] = norm_held[1]
        placed = pltpu.roll(norm_rows[...], 24 * place.data, 1)
        norm_pair[xh, 0] = norm_grad[...]
        norm_pair[xh, 1] = placed[1:2]
        norm_pair[xh, 2] = placed[2:3]

        def share(mine, axis, size):
            arrived = sender.landing()
            sender.begin(size)
            for step in (2,) if axis == "x" else (1, 2, 3):
                sender.start(mine, mine, axis, step, arrived)
            yield
            wait_for(size, arrived)

        yield from share(norm_pair.at[xh], "x", norm_pair.at[0])
        norm_ring[0, y] = norm_pair[0] + norm_pair[1]
        yield from share(norm_ring.at[0, y], "y", norm_ring.at[0, 0:3])
        norm_ring[1, z] = norm_ring[0, 0] + norm_ring[0, 1] + norm_ring[0, 2] + norm_ring[0, 3]
        yield from share(norm_ring.at[1, z], "z", norm_ring.at[1, 0:3])
        total = norm_ring[1, 0] + norm_ring[1, 1] + norm_ring[1, 2] + norm_ring[1, 3]
        new, state = updated(total[0] * mean_rate, total[1], total[2])
        norm_all[...] = new
        norm_rows[0:1] = new
        norm_rows[1:2] = state
        own = pltpu.roll(norm_rows[...], lax.rem(768 - 24 * place.data, 768), 1)
        new_norm[...] = own[0:1, 0:24]
        state_norm[...] = own[1:2, 0:24]

    senders, streams = [], []
    first = 0
    for n, piece in enumerate(STREAMS + (None,)):
        senders.append(Sender(place, send_sems, recv_sems, (2 * n, first)))
        if piece is None:
            streams.append(norm_stream(senders[n]))
        else:
            streams.append(stream(senders[n], *piece, landings[4 * n : 4 * n + 4]))
            first += waits_of(*piece[4:])
    make_ready(UP, 0)
    pl.semaphore_wait(barrier, 7)
    for n in ORDER:
        next(streams[n], None)
    for sender in senders:
        sender.finish()


def waits_of(axes, scatter_modes, gather_modes):
    return 6 + (scatter_modes + gather_modes).count("t")


def landing_shapes():
    shapes = []
    for _, _, _, count, axes, scatter_modes, _ in STREAMS:
        lines = Lines.__new__(Lines)
        lines.axes = axes
        first_shape = (4 if axes[0] == "x" else 6, 3, count, WIDE)
        shapes += [pltpu.VMEM(first_shape, jnp.float32)] * 2
        for stage in (1, 2):
            twice = axes[stage] != "x" and scatter_modes[stage] == "t"
            slots = 1 if axes[stage] == "x" else 6 if twice else 3
            shapes.append(pltpu.VMEM((slots,) + lines.span(stage, twice) + (count, WIDE), jnp.float32))
    return shapes


def split_kernel(up, down, mixed, norm_all, *rest):
    kept, (copy_up, copy_down, *heads, copy_norm), others, sems = rest[:14], rest[14:21], rest[21:35], rest[35]
    pairs = [(up, copy_up), (down, copy_down)]
    pairs += [(mixed.at[pl.ds(192 * n, 192), :], head) for n, head in enumerate(heads)]
    pairs += list(zip(kept, others))
    copies = [pltpu.make_async_copy(source, target, sems.at[n]) for n, (source, target) in enumerate(pairs)]
    for copy in copies:
        copy.start()
    copy_norm[...] = norm_all[0].astype(jnp.bfloat16)
    for copy in copies:
        copy.wait()


def on_device(
    grad_up, grad_down, grad_query, grad_key, grad_value, grad_mixed, grad_norm,
    weight_up, weight_down, weight_query, weight_key, weight_value, weight_mixed, weight_norm,
    moment_up, moment_down, moment_query, moment_key, moment_value, moment_mixed, moment_norm,
):
    f32, bf16 = jnp.float32, jnp.bfloat16
    anywhere = pl.BlockSpec(memory_space=pl.ANY)
    shape = jax.ShapeDtypeStruct
    operands = (
        grad_up[0].reshape(4, 4, 2, 24, 768), grad_down[0],
        grad_query[0].T, grad_key[0].T, grad_value[0].T, grad_mixed[0], grad_norm,
        weight_up, weight_down.T, weight_query, weight_key, weight_value, weight_mixed.T, weight_norm[None],
        moment_up, moment_down.T, moment_query, moment_key, moment_value, moment_mixed.T, moment_norm[None],
    )
    vmem = pl.BlockSpec(memory_space=pltpu.VMEM)
    kept_shapes = ((24, 768),) * 2 + ((24, 192),) * 4 + ((1, 24),)
    inner = (pltpu.VMEM((768, 768), bf16),) * 3 + (pltpu.VMEM((1, 768), f32),)
    inner += tuple(pltpu.VMEM(s, f32) for s in kept_shapes * 2)
    results = pl.pallas_call(
        exchange_kernel,
        name="exchange",
        out_shape=inner,
        in_specs=[anywhere] * 21,
        out_specs=[vmem] * 18,
        scratch_shapes=[
            pltpu.VMEM((3, BLOCKS) + FOLDED, f32),
            pltpu.VMEM((2, 768, 768), f32),
            pltpu.VMEM((2, 3, 24, 768), f32),
            pltpu.VMEM((2, 4, 24, 192), f32),
            pltpu.VMEM((3, BLOCKS, 4, 4, 2, 48, HALF), bf16),
            pltpu.VMEM((2, 24, 768), f32),
            pltpu.VMEM((1, 768), f32),
            pltpu.VMEM((2, 1, 24), f32),
            pltpu.VMEM((8, 768), f32),
            pltpu.VMEM((2, 3, 1, 768), f32),
            pltpu.VMEM((2, 4, 3, 1, 768), f32),
            pltpu.SemaphoreType.DMA((2 * len(STREAMS) + 2,)),
            pltpu.SemaphoreType.DMA((sum(waits_of(*piece[4:]) for piece in STREAMS) + 3,)),
            pltpu.SemaphoreType.DMA((15,)),
        ]
        + landing_shapes(),
        compiler_params=pltpu.CompilerParams(
            collective_id=0, has_side_effects=True, vmem_limit_bytes=56 * 2**20
        ),
    )(*operands)
    outs = pl.pallas_call(
        split_kernel,
        name="split",
        out_shape=(shape((768, 768), bf16),) * 2
        + (shape((192, 768), bf16),) * 4
        + (shape((768,), bf16),)
        + tuple(shape(s, f32) for s in kept_shapes * 2),
        in_specs=[vmem] * 18,
        out_specs=[anywhere] * 6 + [vmem] + [anywhere] * 14,
        scratch_shapes=[pltpu.SemaphoreType.DMA((20,))],
        compiler_params=pltpu.CompilerParams(vmem_limit_bytes=8 * 2**20),
    )(*results)
    copy_up, copy_down, copy_query, copy_key, copy_value, copy_mixed, copy_norm = outs[:7]

    def as_given(seven):
        up, down, query, key, value, mixed, norm = seven
        return (up, down.T, query, key, value, mixed.T, norm[0])

    return (
        (copy_up, copy_down, copy_query.T, copy_key.T, copy_value.T, copy_mixed, copy_norm)
        + as_given(outs[7:14])
        + as_given(outs[14:])
    )


def solution(mesh):
    return jax.shard_map(
        on_device,
        mesh=mesh,
        in_specs=(
            P("data", None, "width"),
            P("data", "width", None),
            P("data", None, "width"),
            P("data", None, "width"),
            P("data", None, "width"),
            P("data", "width", None),
            P("data", None),
        )
        + (
            P("data", "width"),
            P("width", "data"),
            P("data", "width"),
            P("data", "width"),
            P("data", "width"),
            P("width", "data"),
            P("data"),
        )
        * 2,
        out_specs=(
            P(None, "width"),
            P("width", None),
            P(None, "width"),
            P(None, "width"),
            P(None, "width"),
            P("width", None),
            P(),
        )
        + (
            P("data", "width"),
            P("width", "data"),
            P("data", "width"),
            P("data", "width"),
            P("data", "width"),
            P("width", "data"),
            P("data"),
        )
        * 2,
        check_vma=False,
    )
```

```python
import jax
import jax.numpy as jnp
from jax import lax
from jax.experimental import pallas as pl
from jax.experimental.pallas import tpu as pltpu
from jax.sharding import PartitionSpec as P

learn_rate = 0.05
hold_rate = 0.9
mean_rate = 32 ** (-0.5)

MESH = pl.DeviceIdType.MESH
WIDE = 256
HALF = 128
UP, DOWN, MIXED = 0, 1, 2
FOLDED = (4, 4, 2, 24, WIDE)
BLOCKS = 3
RAW = 6.0
STREAMS = (
    (UP, 0, 0, 24, "zxy", "tdd", "tdd"),
    (DOWN, 0, 0, 24, "xyz", "dtd", "ddd"),
    (MIXED, 0, 0, 24, "xyz", "dtd", "ddd"),
    (UP, 1, 0, 24, "yxz", "tdd", "tdd"),
    (DOWN, 1, 0, 24, "yzx", "ttd", "tdd"),
    (MIXED, 1, 0, 24, "zyx", "tdd", "tdd"),
    (UP, 2, 0, 24, "zxy", "tdd", "tdd"),
    (DOWN, 2, 0, 24, "yzx", "tdd", "tdd"),
    (MIXED, 2, 0, 24, "zxy", "tdd", "tdd"),
)
ORDER = (
    0, 3, 6, 1, 2, 4, 5, 7, 8, 9, 0, 3, 6, 4, 1, 5, 7, 8, 3, 4, 2, 0, 9, 1,
    6, 7, 5, 3, 8, 2, 4, 9, 0, 1, 7, 6, 5, 3, 4, 2, 9, 8, 0, 1, 7, 6, 5, 3,
    4, 2, 8, 0, 1, 7, 6, 5, 3, 4, 2, 8, 0, 7, 1, 6, 5, 4, 3, 8, 0, 2, 6, 7,
    5, 1, 4, 8, 3, 7, 0, 6, 2, 4, 5, 8,
)


def on_ring(step, size=4):
    return lax.rem(step, size)


class Place:
    def __init__(self):
        data, width = lax.axis_index("data"), lax.axis_index("width")
        self.z, self.y, self.xh = lax.div(data, 8), lax.rem(lax.div(data, 2), 4), lax.rem(data, 2)
        self.x, self.core = 2 * self.xh + lax.div(width, 2), lax.rem(width, 2)
        self.data = data

    def device(self, z, y, x):
        return (z * 8 + y * 2 + lax.div(x, 2), 2 * lax.rem(x, 2) + self.core)

    def along(self, axis, step):
        z, y, x = self.z, self.y, self.x
        if axis == "z":
            z = on_ring(z + step)
        elif axis == "y":
            y = on_ring(y + step)
        else:
            x = on_ring(x + step)
        return self.device(z, y, x)


class Sender:
    def __init__(self, place, send_sems, recv_sems, first):
        self.place, self.send_sems, self.recv_sems = place, send_sems, recv_sems
        self.next_send, self.next_recv = first
        self.sent = []
        self.turn = 0

    def landing(self):
        self.next_recv += 1
        return self.recv_sems.at[self.next_recv - 1]

    def begin(self, size):
        sem = self.send_sems.at[self.next_send + self.turn]
        self.turn = 1 - self.turn
        if len(self.sent) == 2:
            wait_for(*self.sent.pop(0))
        self.sent.append((size, sem))

    def start(self, source, target, axis, step, landing):
        pltpu.make_async_remote_copy(
            src_ref=source,
            dst_ref=target,
            send_sem=self.sent[-1][1],
            recv_sem=landing,
            device_id=self.place.along(axis, step),
            device_id_type=MESH,
        ).start()

    def finish(self):
        for size, sem in self.sent:
            wait_for(size, sem)


def wait_for(size, sem):
    pltpu.make_async_copy(size, size, sem).wait()


def add_to(ref, *others):
    total = ref[...]
    for other in others:
        total = total + other[...]
    ref[...] = total


class Lines:
    def __init__(self, place, axes):
        self.at = {"z": place.z, "y": place.y, "x": place.xh}
        self.axes = axes

    def chosen(self, stage, q, half=None):
        index = dict(z=slice(None), y=slice(None), x=slice(None))
        for axis in self.axes[:stage]:
            index[axis] = self.at[axis]
        index[self.axes[stage]] = q
        if half is not None:
            split = self.axes[stage + 1] if self.axes[stage + 1] != "x" else self.axes[-1]
            index[split] = half if split == "x" else pl.ds(2 * half, 2)
        return index["z"], index["y"], index["x"]

    def span(self, stage, halved=False):
        sizes = dict(z=4, y=4, x=2)
        left = list(self.axes[stage + 1 :])
        shape = []
        split = None
        if halved:
            split = self.axes[stage + 1] if self.axes[stage + 1] != "x" else self.axes[-1]
        for axis in "zyx":
            if axis in left:
                if axis == split:
                    if axis != "x":
                        shape.append(2)
                else:
                    shape.append(sizes[axis])
        return tuple(shape)


def encode(values, largest):
    if values.shape[-2] == 24:
        return three_as_two(values[:, 0:8], values[:, 8:16], values[:, 16:24], largest)
    return four_as_three(values, largest)


def decode(coded, largest):
    if coded.shape[0] == 4:
        return three_of_two(coded[:, 0:8], coded[:, 8:16], largest)
    return four_of_three(coded, largest)


def three_as_two(one, two, third, largest):
    steps = jnp.floor(third * (127000 / largest) + 127008.5)
    high = jnp.floor((steps + 0.5) * (1 / 504))
    both = []
    for value, digit in ((one, high), (two, steps - high * 504.0)):
        level = jnp.floor((digit + 0.5) * (1 / 63))
        beside = digit - level * 63.0 + 1.0
        top = level >= 4.0
        rest = jnp.where(top, level - 4.0, level)
        middle = rest >= 2.0
        rest = jnp.where(middle, rest - 2.0, rest)
        power = jnp.where(top, 2.0**-25, 2.0**-125)
        power = jnp.where(middle, power * 2.0**50, power)
        power = jnp.where(rest >= 1.0, power * 2.0**25, power)
        whole = jnp.floor(value * ((2**18 - 1) / largest) + 0.5) * 64.0
        both.append((whole + beside) * power)
    return jnp.concatenate(both, axis=1)


def three_of_two(one, two, largest):
    values, digits = [], []
    for coded in (one, two):
        size = jnp.abs(coded)
        top = size >= 2.0**-25
        power = jnp.where(top, 2.0**25, 2.0**125)
        size = size * power
        middle = size >= 2.0**50
        down = jnp.where(middle, 2.0**-50, 1.0)
        size, power = size * down, power * down
        low = size >= 2.0**25
        whole = coded * jnp.where(low, power * 2.0**-25, power)
        level = jnp.where(top, 4.0, 0.0) + jnp.where(middle, 2.0, 0.0) + jnp.where(low, 1.0, 0.0)
        value = jnp.floor(whole * 2.0**-6)
        digits.append(level * 63.0 + (whole - value * 64.0 - 1.0))
        values.append(value * (largest / (2**18 - 1)))
    third = (digits[0] * 504.0 + digits[1] - 127008.0) * (largest / 127000)
    return jnp.concatenate(values + [third], axis=1)


def four_as_three(values, largest):
    first = jnp.floor(values[:3] * ((2**18 - 1) / largest) + 0.5) * 64.0
    fourth = jnp.floor(values[3] * ((2**17 - 1) / largest) + (2**17 + 0.5))
    high = jnp.floor(fourth * 2.0**-12)
    rest = fourth - high * 4096.0
    middle = jnp.floor(rest * 2.0**-6)
    return first + jnp.stack([high, middle, rest - middle * 64.0])


def four_of_three(coded, largest):
    first = jnp.floor(coded * 2.0**-6)
    digits = coded - first * 64.0
    fourth = (digits[0] * 64.0 + digits[1]) * 64.0 + (digits[2] - 2.0**17)
    return jnp.concatenate(
        [first * (largest / (2**18 - 1)), (fourth * (largest / (2**17 - 1)))[None]], axis=0
    )


def fours(ref):
    return ref[...].reshape((4,) + ref.shape[-2:])


def coded_stage(sender, lines, block, coded, landing):
    axis = lines.axes[0]
    at = lines.at[axis]
    if axis == "x":
        far = block(*lines.chosen(0, 1 - at))
        own = block(*lines.chosen(0, at))
        for n in range(4):
            coded[n] = encode(far[n], RAW)
        arrived = sender.landing()
        sender.begin(landing)
        sender.start(coded, landing, axis, 2, arrived)
        yield
        wait_for(landing, arrived)
        for n in range(4):
            own[n] = own[n] + decode(landing[n], RAW)
        return
    plus, minus, opposite = on_ring(at + 1), on_ring(at + 3), on_ring(at + 2)

    def part(q, half):
        return block(*lines.chosen(0, q, half))

    far, final = sender.landing(), sender.landing()

    def send(n, values, largest, step, arrived):
        coded[n] = encode(values, largest)
        sender.start(coded.at[n], landing.at[n], axis, step, arrived)

    sender.begin(landing.at[0:4])
    send(0, fours(part(opposite, 0)), RAW, 1, far)
    send(1, fours(part(opposite, 1)), RAW, 3, far)
    send(2, fours(part(plus, 1)), RAW, 1, final)
    send(3, fours(part(minus, 0)), RAW, 3, final)
    yield
    wait_for(landing.at[0:2], far)
    sender.begin(landing.at[4:6])
    send(4, fours(part(plus, 0)) + decode(landing[0], RAW), 2 * RAW, 1, final)
    send(5, fours(part(minus, 1)) + decode(landing[1], RAW), 2 * RAW, 3, final)
    yield
    wait_for(landing.at[2:6], final)
    for near, both, half in ((3, 4, 0), (2, 5, 1)):
        own = part(at, half)
        total = fours(own) + decode(landing[near], RAW) + decode(landing[both], 2 * RAW)
        own[...] = total.reshape(own.shape)


def scatter_stage(sender, lines, stage, mode, block, landing):
    axis = lines.axes[stage]
    at = lines.at[axis]
    own = block(*lines.chosen(stage, at))
    plus, minus, opposite = on_ring(at + 1), on_ring(at + 3), on_ring(at + 2)
    if axis == "x" or mode == "d":
        arrived = sender.landing()
        sender.begin(landing)
        targets = ((1 - at, 2),) if axis == "x" else ((opposite, 2), (plus, 1), (minus, 3))
        for n, (q, step) in enumerate(targets):
            sender.start(block(*lines.chosen(stage, q)), landing.at[n], axis, step, arrived)
        yield
        wait_for(landing, arrived)
        add_to(own, *(landing.at[n] for n in range(len(targets))))
        return

    def part(q, half):
        return block(*lines.chosen(stage, q, half))

    far, final = sender.landing(), sender.landing()
    sender.begin(landing.at[0:4])
    sender.start(part(opposite, 0), landing.at[0], axis, 1, far)
    sender.start(part(opposite, 1), landing.at[1], axis, 3, far)
    sender.start(part(plus, 1), landing.at[2], axis, 1, final)
    sender.start(part(minus, 0), landing.at[3], axis, 3, final)
    yield
    wait_for(landing.at[0:2], far)
    sender.begin(landing.at[4:6])
    add_to(part(plus, 0), landing.at[0])
    sender.start(part(plus, 0), landing.at[4], axis, 1, final)
    add_to(part(minus, 1), landing.at[1])
    sender.start(part(minus, 1), landing.at[5], axis, 3, final)
    yield
    wait_for(landing.at[2:6], final)
    add_to(part(at, 0), landing.at[3], landing.at[4])
    add_to(part(at, 1), landing.at[2], landing.at[5])


def gather_stage(sender, lines, stage, mode, block):
    axis = lines.axes[stage]
    at = lines.at[axis]
    own = block(*lines.chosen(stage, at))
    if axis == "x" or mode == "d":
        steps = (2,) if axis == "x" else (2, 1, 3)
        arrived = sender.landing()
        size = block(*lines.chosen(stage, pl.ds(0, len(steps))))
        sender.begin(size)
        for step in steps:
            sender.start(own, own, axis, step, arrived)
        yield
        wait_for(size, arrived)
        return

    def part(q, half):
        return block(*lines.chosen(stage, q, half))

    plus, minus = on_ring(at + 1), on_ring(at + 3)
    near, final = sender.landing(), sender.landing()
    two = block(*lines.chosen(stage, pl.ds(0, 2)))
    sender.begin(two)
    sender.start(part(at, 0), part(at, 0), axis, 1, near)
    sender.start(part(at, 1), part(at, 1), axis, 3, near)
    sender.start(part(at, 1), part(at, 1), axis, 1, final)
    sender.start(part(at, 0), part(at, 0), axis, 3, final)
    yield
    wait_for(own, near)
    sender.begin(own)
    sender.start(part(minus, 0), part(minus, 0), axis, 1, final)
    sender.start(part(plus, 1), part(plus, 1), axis, 3, final)
    yield
    wait_for(two, final)


def updated(mean, weight, moment):
    state = hold_rate * moment + (1.0 - hold_rate) * mean * mean
    return weight - learn_rate * mean * lax.rsqrt(state + 1e-06), state


def exchange_kernel(*refs):
    (
        grad_up, grad_down, grad_query, grad_key, grad_value, grad_mixed, grad_norm,
        weight_up, weight_down, weight_query, weight_key, weight_value, weight_mixed, weight_norm,
        moment_up, moment_down, moment_query, moment_key, moment_value, moment_mixed, moment_norm,
        out_up, out_down, out_mixed, norm_all,
        new_up, new_down, new_query, new_key, new_value, new_mixed, new_norm,
        state_up, state_down, state_query, state_key, state_value, state_mixed, state_norm,
        sums, turned, held, held_heads, whole, mixed_own,
        norm_grad, norm_held, norm_rows, norm_pair, norm_ring,
        send_sems, recv_sems, load_sems,
        *landings,
    ) = refs
    place = Place()
    z, y, xh = place.z, place.y, place.xh
    columns = [pl.ds(WIDE * k, WIDE) for k in range(BLOCKS)]

    barrier = pltpu.get_barrier_semaphore()
    for axis in ("x", "y", "z"):
        for step in (2,) if axis == "x" else (1, 2, 3):
            pl.semaphore_signal(barrier, inc=1, device_id=place.along(axis, step), device_id_type=MESH)

    loads = {}

    def load(name, *pairs, size=None):
        sem = load_sems.at[len(loads)]
        for source, target in pairs:
            pltpu.make_async_copy(source, target, sem).start()
        loads[name] = pairs[0][1] if size is None else size, sem

    def loaded(name):
        wait_for(*loads[name])

    heads = (grad_query, grad_key, grad_value, grad_mixed)
    for k in range(BLOCKS):
        load((UP, k), (grad_up.at[:, :, :, :, columns[k]], sums.at[UP, k]))
        load((DOWN, k), (grad_down.at[columns[k], :], turned.at[0, columns[k], :]))
        for head in ((0, 1), (2,), (3,))[k]:
            load(("head", head), (heads[head], turned.at[1, pl.ds(192 * head, 192), :]))
    load("norm", (grad_norm, norm_grad))
    load("held norm", (weight_norm, norm_held.at[0]), (moment_norm, norm_held.at[1]), size=norm_held)
    for part, weight, moment in ((UP, weight_up, moment_up), (DOWN, weight_down, moment_down)):
        load(
            ("held", part), (weight, held.at[0, part]), (moment, held.at[1, part]), size=held.at[:, part]
        )
    four_weights = (weight_query, weight_key, weight_value, weight_mixed)
    four_moments = (moment_query, moment_key, moment_value, moment_mixed)
    load(
        ("held", MIXED),
        *((source, held_heads.at[0, head]) for head, source in enumerate(four_weights)),
        *((source, held_heads.at[1, head]) for head, source in enumerate(four_moments)),
        size=held_heads,
    )

    gathered = {}
    ready = set()

    def make_ready(part, k):
        if (part, k) in ready:
            return
        ready.add((part, k))
        if part == UP:
            loaded((UP, k))
            return
        if part == DOWN:
            loaded((DOWN, k))
        else:
            for head in ((0, 1), (2,), (3,))[k]:
                loaded(("head", head))

        def turn(n, carry):
            lanes = pl.ds(pl.multiple_of(384 * n, HALF), 384)
            tile = turned[part - 1, columns[k], lanes]
            sums[part, k, pl.ds(2 * n, 2)] = tile.T.reshape(2, 4, 2, 24, WIDE)
            return carry

        lax.fori_loop(0, 2, turn, 0)

    def hold(part):
        if ("held", part) in ready:
            return
        ready.add(("held", part))
        loaded(("held", part))
        if part == MIXED:
            for row in range(2):
                held[row, part] = jnp.concatenate([held_heads[row, head] for head in range(4)], axis=1)

    def finish(part, k, rows):
        done = gathered.setdefault((part, k), [])
        done.append(rows)
        if sum(count for _, count in done) < 24:
            return
        done.sort()

        def side(chunk, half):
            return [
                chunk[..., 2 * first + count * half : 2 * first + count * half + count, :]
                for first, count in done
            ]

        if part == UP:

            def pair_of_chunks(n, carry):
                chunks = [
                    whole[UP, k, lax.div(n, 4), lax.rem(n, 4), c].astype(jnp.float32) for c in range(2)
                ]
                at = pl.ds(pl.multiple_of(48 * n, 16), 48)
                for half in range(2):
                    both = jnp.concatenate(side(chunks[0], half) + side(chunks[1], half), axis=0)
                    out_up[at, pl.ds(WIDE * k + HALF * half, HALF)] = both.astype(jnp.bfloat16)
                return carry

            lax.fori_loop(0, 16, pair_of_chunks, 0)
            return
        for half in range(2):
            chunks = whole[part, k].astype(jnp.float32)
            tile = jnp.concatenate(side(chunks, half), axis=-2)
            (out_down, out_mixed)[part - 1][pl.ds(WIDE * k + HALF * half, HALF), :] = (
                tile.reshape(768, HALF).T.astype(jnp.bfloat16)
            )

    def keep(part, k, rows, new, state):
        if part != MIXED:
            (new_up, new_down)[part][rows, columns[k]] = new
            (state_up, state_down)[part][rows, columns[k]] = state
            return
        mixed_own[0, rows, columns[k]] = new
        mixed_own[1, rows, columns[k]] = state
        gathered["kept"] = gathered.get("kept", 0) + 1
        if gathered["kept"] == sum(piece[0] == MIXED for piece in STREAMS):
            for row, targets in enumerate(
                ((new_query, new_key, new_value, new_mixed), (state_query, state_key, state_value, state_mixed))
            ):
                everything = mixed_own[row]
                for head in range(4):
                    targets[head][...] = everything[:, 192 * head : 192 * head + 192]

    def stream(sender, part, k, first, count, axes, scatter_modes, gather_modes, lands):
        rows = pl.ds(first, count)
        copied = pl.ds(2 * first, 2 * count)
        lines = Lines(place, axes)

        def block(*index):
            return sums.at[(part, k) + index + (rows, slice(None))]

        def copy_block(*index):
            return whole.at[(part, k) + index + (copied, slice(None))]

        make_ready(part, k)
        coded, *lands = lands
        yield from coded_stage(sender, lines, block, coded, lands[0])
        for stage in (1, 2):
            yield from scatter_stage(sender, lines, stage, scatter_modes[stage], block, lands[stage])
        hold(part)
        own = sums[part, k, z, y, xh, rows, :] * mean_rate
        new, state = updated(own, held[0, part, rows, columns[k]], held[1, part, rows, columns[k]])
        keep(part, k, rows, new, state)
        whole[part, k, z, y, xh, copied, :] = jnp.concatenate(
            [new[:, :HALF], new[:, HALF:]], axis=0
        ).astype(jnp.bfloat16)
        for stage in (2, 1, 0):
            yield from gather_stage(sender, lines, stage, gather_modes[stage], copy_block)
        finish(part, k, (first, count))

    def norm_stream(sender):
        loaded("norm")
        loaded("held norm")
        norm_rows[...] = jnp.zeros_like(norm_rows)
        norm_rows[1:2, 0:24] = norm_held[0]
        norm_rows[2:3, 0:24] = norm_held[1]
        placed = pltpu.roll(norm_rows[...], 24 * place.data, 1)
        norm_pair[xh, 0] = norm_grad[...]
        norm_pair[xh, 1] = placed[1:2]
        norm_pair[xh, 2] = placed[2:3]

        def share(mine, axis, size):
            arrived = sender.landing()
            sender.begin(size)
            for step in (2,) if axis == "x" else (1, 2, 3):
                sender.start(mine, mine, axis, step, arrived)
            yield
            wait_for(size, arrived)

        yield from share(norm_pair.at[xh], "x", norm_pair.at[0])
        norm_ring[0, y] = norm_pair[0] + norm_pair[1]
        yield from share(norm_ring.at[0, y], "y", norm_ring.at[0, 0:3])
        norm_ring[1, z] = norm_ring[0, 0] + norm_ring[0, 1] + norm_ring[0, 2] + norm_ring[0, 3]
        yield from share(norm_ring.at[1, z], "z", norm_ring.at[1, 0:3])
        total = norm_ring[1, 0] + norm_ring[1, 1] + norm_ring[1, 2] + norm_ring[1, 3]
        new, state = updated(total[0] * mean_rate, total[1], total[2])
        norm_all[...] = new
        norm_rows[0:1] = new
        norm_rows[1:2] = state
        own = pltpu.roll(norm_rows[...], lax.rem(768 - 24 * place.data, 768), 1)
        new_norm[...] = own[0:1, 0:24]
        state_norm[...] = own[1:2, 0:24]

    senders, streams = [], []
    first = 0
    for n, piece in enumerate(STREAMS + (None,)):
        senders.append(Sender(place, send_sems, recv_sems, (2 * n, first)))
        if piece is None:
            streams.append(norm_stream(senders[n]))
        else:
            streams.append(stream(senders[n], *piece, landings[4 * n : 4 * n + 4]))
            first += waits_of(*piece[4:])
    make_ready(UP, 0)
    pl.semaphore_wait(barrier, 7)
    for n in ORDER:
        next(streams[n], None)
    for sender in senders:
        sender.finish()


def waits_of(axes, scatter_modes, gather_modes):
    return 6 + (scatter_modes + gather_modes).count("t")


def landing_shapes():
    shapes = []
    for _, _, _, count, axes, scatter_modes, _ in STREAMS:
        lines = Lines.__new__(Lines)
        lines.axes = axes
        coded_shape = (4, 16, WIDE) if count == 24 else (3, count, WIDE)
        first_shape = (4 if axes[0] == "x" else 6,) + coded_shape
        shapes += [pltpu.VMEM(first_shape, jnp.float32)] * 2
        for stage in (1, 2):
            twice = axes[stage] != "x" and scatter_modes[stage] == "t"
            slots = 1 if axes[stage] == "x" else 6 if twice else 3
            shapes.append(pltpu.VMEM((slots,) + lines.span(stage, twice) + (count, WIDE), jnp.float32))
    return shapes


def split_kernel(up, down, mixed, norm_all, *rest):
    kept, (copy_up, copy_down, *heads, copy_norm), others, sems = rest[:14], rest[14:21], rest[21:35], rest[35]
    pairs = [(up, copy_up), (down, copy_down)]
    pairs += [(mixed.at[pl.ds(192 * n, 192), :], head) for n, head in enumerate(heads)]
    pairs += list(zip(kept, others))
    copies = [pltpu.make_async_copy(source, target, sems.at[n]) for n, (source, target) in enumerate(pairs)]
    for copy in copies:
        copy.start()
    copy_norm[...] = norm_all[0].astype(jnp.bfloat16)
    for copy in copies:
        copy.wait()


def on_device(
    grad_up, grad_down, grad_query, grad_key, grad_value, grad_mixed, grad_norm,
    weight_up, weight_down, weight_query, weight_key, weight_value, weight_mixed, weight_norm,
    moment_up, moment_down, moment_query, moment_key, moment_value, moment_mixed, moment_norm,
):
    f32, bf16 = jnp.float32, jnp.bfloat16
    anywhere = pl.BlockSpec(memory_space=pl.ANY)
    shape = jax.ShapeDtypeStruct
    operands = (
        grad_up[0].reshape(4, 4, 2, 24, 768), grad_down[0],
        grad_query[0].T, grad_key[0].T, grad_value[0].T, grad_mixed[0], grad_norm,
        weight_up, weight_down.T, weight_query, weight_key, weight_value, weight_mixed.T, weight_norm[None],
        moment_up, moment_down.T, moment_query, moment_key, moment_value, moment_mixed.T, moment_norm[None],
    )
    vmem = pl.BlockSpec(memory_space=pltpu.VMEM)
    kept_shapes = ((24, 768),) * 2 + ((24, 192),) * 4 + ((1, 24),)
    inner = (pltpu.VMEM((768, 768), bf16),) * 3 + (pltpu.VMEM((1, 768), f32),)
    inner += tuple(pltpu.VMEM(s, f32) for s in kept_shapes * 2)
    results = pl.pallas_call(
        exchange_kernel,
        name="exchange",
        out_shape=inner,
        in_specs=[anywhere] * 21,
        out_specs=[vmem] * 18,
        scratch_shapes=[
            pltpu.VMEM((3, BLOCKS) + FOLDED, f32),
            pltpu.VMEM((2, 768, 768), f32),
            pltpu.VMEM((2, 3, 24, 768), f32),
            pltpu.VMEM((2, 4, 24, 192), f32),
            pltpu.VMEM((3, BLOCKS, 4, 4, 2, 48, HALF), bf16),
            pltpu.VMEM((2, 24, 768), f32),
            pltpu.VMEM((1, 768), f32),
            pltpu.VMEM((2, 1, 24), f32),
            pltpu.VMEM((8, 768), f32),
            pltpu.VMEM((2, 3, 1, 768), f32),
            pltpu.VMEM((2, 4, 3, 1, 768), f32),
            pltpu.SemaphoreType.DMA((2 * len(STREAMS) + 2,)),
            pltpu.SemaphoreType.DMA((sum(waits_of(*piece[4:]) for piece in STREAMS) + 3,)),
            pltpu.SemaphoreType.DMA((15,)),
        ]
        + landing_shapes(),
        compiler_params=pltpu.CompilerParams(
            collective_id=0, has_side_effects=True, vmem_limit_bytes=56 * 2**20
        ),
    )(*operands)
    outs = pl.pallas_call(
        split_kernel,
        name="split",
        out_shape=(shape((768, 768), bf16),) * 2
        + (shape((192, 768), bf16),) * 4
        + (shape((768,), bf16),)
        + tuple(shape(s, f32) for s in kept_shapes * 2),
        in_specs=[vmem] * 18,
        out_specs=[anywhere] * 6 + [vmem] + [anywhere] * 14,
        scratch_shapes=[pltpu.SemaphoreType.DMA((20,))],
        compiler_params=pltpu.CompilerParams(vmem_limit_bytes=8 * 2**20),
    )(*results)
    copy_up, copy_down, copy_query, copy_key, copy_value, copy_mixed, copy_norm = outs[:7]

    def as_given(seven):
        up, down, query, key, value, mixed, norm = seven
        return (up, down.T, query, key, value, mixed.T, norm[0])

    return (
        (copy_up, copy_down, copy_query.T, copy_key.T, copy_value.T, copy_mixed, copy_norm)
        + as_given(outs[7:14])
        + as_given(outs[14:])
    )


def solution(mesh):
    return jax.shard_map(
        on_device,
        mesh=mesh,
        in_specs=(
            P("data", None, "width"),
            P("data", "width", None),
            P("data", None, "width"),
            P("data", None, "width"),
            P("data", None, "width"),
            P("data", "width", None),
            P("data", None),
        )
        + (
            P("data", "width"),
            P("width", "data"),
            P("data", "width"),
            P("data", "width"),
            P("data", "width"),
            P("width", "data"),
            P("data"),
        )
        * 2,
        out_specs=(
            P(None, "width"),
            P("width", None),
            P(None, "width"),
            P(None, "width"),
            P(None, "width"),
            P("width", None),
            P(),
        )
        + (
            P("data", "width"),
            P("width", "data"),
            P("data", "width"),
            P("data", "width"),
            P("data", "width"),
            P("width", "data"),
            P("data"),
        )
        * 2,
        check_vma=False,
    )
```

```python
import jax
import jax.numpy as jnp
from jax import lax
from jax.experimental import pallas as pl
from jax.experimental.pallas import tpu as pltpu
from jax.sharding import PartitionSpec as P

learn_rate = 0.05
hold_rate = 0.9
mean_rate = 32 ** (-0.5)

MESH = pl.DeviceIdType.MESH
WIDE = 256
HALF = 128
UP, DOWN, MIXED = 0, 1, 2
FOLDED = (4, 4, 2, 24, WIDE)
BLOCKS = 3
RAW = 6.0
STREAMS = (
    (UP, 0, 0, 24, "zxy", "tdd", "tdd"),
    (DOWN, 0, 0, 24, "xyz", "dtd", "ddd"),
    (MIXED, 0, 0, 24, "xyz", "dtd", "ddd"),
    (UP, 1, 0, 24, "yxz", "tdd", "tdd"),
    (DOWN, 1, 0, 24, "yzx", "ttd", "tdd"),
    (MIXED, 1, 0, 24, "zyx", "tdd", "tdd"),
    (UP, 2, 0, 24, "zxy", "tdd", "tdd"),
    (DOWN, 2, 0, 24, "yzx", "tdd", "tdd"),
    (MIXED, 2, 0, 24, "zxy", "tdd", "tdd"),
)
ORDER = (
    0, 3, 6, 1, 2, 4, 5, 7, 8, 9, 0, 3, 6, 4, 1, 5, 7, 8, 3, 4, 2, 0, 9, 1,
    6, 7, 5, 3, 8, 2, 4, 9, 0, 1, 7, 6, 5, 3, 4, 2, 9, 8, 0, 1, 7, 6, 5, 3,
    4, 2, 8, 0, 1, 7, 6, 5, 3, 4, 2, 8, 0, 7, 1, 6, 5, 4, 3, 8, 0, 2, 6, 7,
    5, 1, 4, 8, 3, 7, 0, 6, 2, 4, 5, 8,
)


def on_ring(step, size=4):
    return lax.rem(step, size)


class Place:
    def __init__(self):
        data, width = lax.axis_index("data"), lax.axis_index("width")
        self.z, self.y, self.xh = lax.div(data, 8), lax.rem(lax.div(data, 2), 4), lax.rem(data, 2)
        self.x, self.core = 2 * self.xh + lax.div(width, 2), lax.rem(width, 2)
        self.data = data

    def device(self, z, y, x):
        return (z * 8 + y * 2 + lax.div(x, 2), 2 * lax.rem(x, 2) + self.core)

    def along(self, axis, step):
        z, y, x = self.z, self.y, self.x
        if axis == "z":
            z = on_ring(z + step)
        elif axis == "y":
            y = on_ring(y + step)
        else:
            x = on_ring(x + step)
        return self.device(z, y, x)


class Sender:
    def __init__(self, place, send_sems, recv_sems, first):
        self.place, self.send_sems, self.recv_sems = place, send_sems, recv_sems
        self.next_send, self.next_recv = first
        self.sent = []
        self.turn = 0
        self.taken, self.spare = {}, []

    def scatters(self, stage):
        self.spare, self.taken[stage] = [], []

    def gathers(self, stage):
        self.spare = list(self.taken.get(stage - 1, ()))

    def landing(self):
        if self.spare:
            return self.recv_sems.at[self.spare.pop()]
        self.next_recv += 1
        self.taken[max(self.taken, default=0)] = self.taken.get(max(self.taken, default=0), []) + [self.next_recv - 1]
        return self.recv_sems.at[self.next_recv - 1]

    def begin(self, size):
        sem = self.send_sems.at[self.next_send + self.turn]
        self.turn = 1 - self.turn
        if len(self.sent) == 2:
            wait_for(*self.sent.pop(0))
        self.sent.append((size, sem))

    def start(self, source, target, axis, step, landing):
        pltpu.make_async_remote_copy(
            src_ref=source,
            dst_ref=target,
            send_sem=self.sent[-1][1],
            recv_sem=landing,
            device_id=self.place.along(axis, step),
            device_id_type=MESH,
        ).start()

    def finish(self):
        for size, sem in self.sent:
            wait_for(size, sem)


def wait_for(size, sem):
    pltpu.make_async_copy(size, size, sem).wait()


def add_to(ref, *others):
    total = ref[...]
    for other in others:
        total = total + other[...]
    ref[...] = total


class Lines:
    def __init__(self, place, axes):
        self.at = {"z": place.z, "y": place.y, "x": place.xh}
        self.axes = axes

    def chosen(self, stage, q, half=None):
        index = dict(z=slice(None), y=slice(None), x=slice(None))
        for axis in self.axes[:stage]:
            index[axis] = self.at[axis]
        index[self.axes[stage]] = q
        if half is not None:
            split = self.axes[stage + 1] if self.axes[stage + 1] != "x" else self.axes[-1]
            index[split] = half if split == "x" else pl.ds(2 * half, 2)
        return index["z"], index["y"], index["x"]

    def span(self, stage, halved=False):
        sizes = dict(z=4, y=4, x=2)
        left = list(self.axes[stage + 1 :])
        shape = []
        split = None
        if halved:
            split = self.axes[stage + 1] if self.axes[stage + 1] != "x" else self.axes[-1]
        for axis in "zyx":
            if axis in left:
                if axis == split:
                    if axis != "x":
                        shape.append(2)
                else:
                    shape.append(sizes[axis])
        return tuple(shape)


def encode(values, largest):
    if values.shape[-2] == 24:
        return three_as_two(values[:, 0:8], values[:, 8:16], values[:, 16:24], largest)
    return four_as_three(values, largest)


def decode(coded, largest):
    if coded.shape[0] == 4:
        return three_of_two(coded[:, 0:8], coded[:, 8:16], largest)
    return four_of_three(coded, largest)


def three_as_two(one, two, third, largest):
    steps = jnp.floor(third * (127000 / largest) + 127008.5)
    high = jnp.floor((steps + 0.5) * (1 / 504))
    both = []
    for value, digit in ((one, high), (two, steps - high * 504.0)):
        level = jnp.floor((digit + 0.5) * (1 / 63))
        beside = digit - level * 63.0 + 1.0
        top = level >= 4.0
        rest = jnp.where(top, level - 4.0, level)
        middle = rest >= 2.0
        rest = jnp.where(middle, rest - 2.0, rest)
        power = jnp.where(top, 2.0**-25, 2.0**-125)
        power = jnp.where(middle, power * 2.0**50, power)
        power = jnp.where(rest >= 1.0, power * 2.0**25, power)
        whole = jnp.floor(value * ((2**18 - 1) / largest) + 0.5) * 64.0
        both.append((whole + beside) * power)
    return jnp.concatenate(both, axis=1)


def three_of_two(one, two, largest):
    values, digits = [], []
    for coded in (one, two):
        size = jnp.abs(coded)
        top = size >= 2.0**-25
        power = jnp.where(top, 2.0**25, 2.0**125)
        size = size * power
        middle = size >= 2.0**50
        down = jnp.where(middle, 2.0**-50, 1.0)
        size, power = size * down, power * down
        low = size >= 2.0**25
        whole = coded * jnp.where(low, power * 2.0**-25, power)
        level = jnp.where(top, 4.0, 0.0) + jnp.where(middle, 2.0, 0.0) + jnp.where(low, 1.0, 0.0)
        value = jnp.floor(whole * 2.0**-6)
        digits.append(level * 63.0 + (whole - value * 64.0 - 1.0))
        values.append(value * (largest / (2**18 - 1)))
    third = (digits[0] * 504.0 + digits[1] - 127008.0) * (largest / 127000)
    return jnp.concatenate(values + [third], axis=1)


def four_as_three(values, largest):
    first = jnp.floor(values[:3] * ((2**18 - 1) / largest) + 0.5) * 64.0
    fourth = jnp.floor(values[3] * ((2**17 - 1) / largest) + (2**17 + 0.5))
    high = jnp.floor(fourth * 2.0**-12)
    rest = fourth - high * 4096.0
    middle = jnp.floor(rest * 2.0**-6)
    return first + jnp.stack([high, middle, rest - middle * 64.0])


def four_of_three(coded, largest):
    first = jnp.floor(coded * 2.0**-6)
    digits = coded - first * 64.0
    fourth = (digits[0] * 64.0 + digits[1]) * 64.0 + (digits[2] - 2.0**17)
    return jnp.concatenate(
        [first * (largest / (2**18 - 1)), (fourth * (largest / (2**17 - 1)))[None]], axis=0
    )


def fours(ref):
    return ref[...].reshape((4,) + ref.shape[-2:])


def coded_stage(sender, lines, block, coded, landing):
    axis = lines.axes[0]
    at = lines.at[axis]
    if axis == "x":
        far = block(*lines.chosen(0, 1 - at))
        own = block(*lines.chosen(0, at))
        for n in range(4):
            coded[n] = encode(far[n], RAW)
        arrived = sender.landing()
        sender.begin(landing)
        sender.start(coded, landing, axis, 2, arrived)
        yield
        wait_for(landing, arrived)
        for n in range(4):
            own[n] = own[n] + decode(landing[n], RAW)
        return
    plus, minus, opposite = on_ring(at + 1), on_ring(at + 3), on_ring(at + 2)

    def part(q, half):
        return block(*lines.chosen(0, q, half))

    far, final = sender.landing(), sender.landing()

    def send(n, values, largest, step, arrived):
        coded[n] = encode(values, largest)
        sender.start(coded.at[n], landing.at[n], axis, step, arrived)

    sender.begin(landing.at[0:4])
    send(0, fours(part(opposite, 0)), RAW, 1, far)
    send(1, fours(part(opposite, 1)), RAW, 3, far)
    send(2, fours(part(plus, 1)), RAW, 1, final)
    send(3, fours(part(minus, 0)), RAW, 3, final)
    yield
    wait_for(landing.at[0:2], far)
    sender.begin(landing.at[4:6])
    send(4, fours(part(plus, 0)) + decode(landing[0], RAW), 2 * RAW, 1, final)
    send(5, fours(part(minus, 1)) + decode(landing[1], RAW), 2 * RAW, 3, final)
    yield
    wait_for(landing.at[2:6], final)
    for near, both, half in ((3, 4, 0), (2, 5, 1)):
        own = part(at, half)
        total = fours(own) + decode(landing[near], RAW) + decode(landing[both], 2 * RAW)
        own[...] = total.reshape(own.shape)


def scatter_stage(sender, lines, stage, mode, block, landing):
    axis = lines.axes[stage]
    at = lines.at[axis]
    own = block(*lines.chosen(stage, at))
    plus, minus, opposite = on_ring(at + 1), on_ring(at + 3), on_ring(at + 2)
    if axis == "x" or mode == "d":
        arrived = sender.landing()
        sender.begin(landing)
        targets = ((1 - at, 2),) if axis == "x" else ((opposite, 2), (plus, 1), (minus, 3))
        for n, (q, step) in enumerate(targets):
            sender.start(block(*lines.chosen(stage, q)), landing.at[n], axis, step, arrived)
        yield
        wait_for(landing, arrived)
        add_to(own, *(landing.at[n] for n in range(len(targets))))
        return

    def part(q, half):
        return block(*lines.chosen(stage, q, half))

    far, final = sender.landing(), sender.landing()
    sender.begin(landing.at[0:4])
    sender.start(part(opposite, 0), landing.at[0], axis, 1, far)
    sender.start(part(opposite, 1), landing.at[1], axis, 3, far)
    sender.start(part(plus, 1), landing.at[2], axis, 1, final)
    sender.start(part(minus, 0), landing.at[3], axis, 3, final)
    yield
    wait_for(landing.at[0:2], far)
    sender.begin(landing.at[4:6])
    add_to(part(plus, 0), landing.at[0])
    sender.start(part(plus, 0), landing.at[4], axis, 1, final)
    add_to(part(minus, 1), landing.at[1])
    sender.start(part(minus, 1), landing.at[5], axis, 3, final)
    yield
    wait_for(landing.at[2:6], final)
    add_to(part(at, 0), landing.at[3], landing.at[4])
    add_to(part(at, 1), landing.at[2], landing.at[5])


def gather_stage(sender, lines, stage, mode, block):
    axis = lines.axes[stage]
    at = lines.at[axis]
    own = block(*lines.chosen(stage, at))
    if axis == "x" or mode == "d":
        steps = (2,) if axis == "x" else (2, 1, 3)
        arrived = sender.landing()
        size = block(*lines.chosen(stage, pl.ds(0, len(steps))))
        sender.begin(size)
        for step in steps:
            sender.start(own, own, axis, step, arrived)
        yield
        wait_for(size, arrived)
        return

    def part(q, half):
        return block(*lines.chosen(stage, q, half))

    plus, minus = on_ring(at + 1), on_ring(at + 3)
    near, final = sender.landing(), sender.landing()
    two = block(*lines.chosen(stage, pl.ds(0, 2)))
    sender.begin(two)
    sender.start(part(at, 0), part(at, 0), axis, 1, near)
    sender.start(part(at, 1), part(at, 1), axis, 3, near)
    sender.start(part(at, 1), part(at, 1), axis, 1, final)
    sender.start(part(at, 0), part(at, 0), axis, 3, final)
    yield
    wait_for(own, near)
    sender.begin(own)
    sender.start(part(minus, 0), part(minus, 0), axis, 1, final)
    sender.start(part(plus, 1), part(plus, 1), axis, 3, final)
    yield
    wait_for(two, final)


def updated(mean, weight, moment):
    state = hold_rate * moment + (1.0 - hold_rate) * mean * mean
    return weight - learn_rate * mean * lax.rsqrt(state + 1e-06), state


def exchange_kernel(*refs):
    (
        grad_up, grad_down, grad_query, grad_key, grad_value, grad_mixed, grad_norm,
        weight_up, weight_down, weight_query, weight_key, weight_value, weight_mixed, weight_norm,
        moment_up, moment_down, moment_query, moment_key, moment_value, moment_mixed, moment_norm,
        out_up, out_down, out_mixed, norm_all,
        new_up, new_down, new_query, new_key, new_value, new_mixed, new_norm,
        state_up, state_down, state_query, state_key, state_value, state_mixed, state_norm,
        sums, turned, held, held_heads, whole, mixed_own,
        norm_grad, norm_held, norm_rows, norm_pair, norm_ring,
        send_sems, recv_sems, load_sems,
        *landings,
    ) = refs
    place = Place()
    z, y, xh = place.z, place.y, place.xh
    columns = [pl.ds(WIDE * k, WIDE) for k in range(BLOCKS)]

    barrier = pltpu.get_barrier_semaphore()
    for axis in ("x", "y", "z"):
        for step in (2,) if axis == "x" else (1, 2, 3):
            pl.semaphore_signal(barrier, inc=1, device_id=place.along(axis, step), device_id_type=MESH)

    loads = {}

    def load(name, *pairs, size=None):
        sem = load_sems.at[len(loads)]
        for source, target in pairs:
            pltpu.make_async_copy(source, target, sem).start()
        loads[name] = pairs[0][1] if size is None else size, sem

    def loaded(name):
        wait_for(*loads[name])

    heads = (grad_query, grad_key, grad_value, grad_mixed)
    for k in range(BLOCKS):
        load((UP, k), (grad_up.at[:, :, :, :, columns[k]], sums.at[UP, k]))
        load((DOWN, k), (grad_down.at[columns[k], :], turned.at[0, columns[k], :]))
        for head in ((0, 1), (2,), (3,))[k]:
            load(("head", head), (heads[head], turned.at[1, pl.ds(192 * head, 192), :]))
    load("norm", (grad_norm, norm_grad))
    load("held norm", (weight_norm, norm_held.at[0]), (moment_norm, norm_held.at[1]), size=norm_held)
    for part, weight, moment in ((UP, weight_up, moment_up), (DOWN, weight_down, moment_down)):
        load(
            ("held", part), (weight, held.at[0, part]), (moment, held.at[1, part]), size=held.at[:, part]
        )
    four_weights = (weight_query, weight_key, weight_value, weight_mixed)
    four_moments = (moment_query, moment_key, moment_value, moment_mixed)
    load(
        ("held", MIXED),
        *((source, held_heads.at[0, head]) for head, source in enumerate(four_weights)),
        *((source, held_heads.at[1, head]) for head, source in enumerate(four_moments)),
        size=held_heads,
    )

    gathered = {}
    ready = set()

    def make_ready(part, k):
        if (part, k) in ready:
            return
        ready.add((part, k))
        if part == UP:
            loaded((UP, k))
            return
        if part == DOWN:
            loaded((DOWN, k))
        else:
            for head in ((0, 1), (2,), (3,))[k]:
                loaded(("head", head))

        def turn(n, carry):
            lanes = pl.ds(pl.multiple_of(384 * n, HALF), 384)
            tile = turned[part - 1, columns[k], lanes]
            sums[part, k, pl.ds(2 * n, 2)] = tile.T.reshape(2, 4, 2, 24, WIDE)
            return carry

        lax.fori_loop(0, 2, turn, 0)

    def hold(part):
        if ("held", part) in ready:
            return
        ready.add(("held", part))
        loaded(("held", part))
        if part == MIXED:
            for row in range(2):
                held[row, part] = jnp.concatenate([held_heads[row, head] for head in range(4)], axis=1)

    def finish(part, k, rows):
        done = gathered.setdefault((part, k), [])
        done.append(rows)
        if sum(count for _, count in done) < 24:
            return
        done.sort()

        def side(chunk, half):
            return [
                chunk[..., 2 * first + count * half : 2 * first + count * half + count, :]
                for first, count in done
            ]

        if part == UP:

            def pair_of_chunks(n, carry):
                chunks = [
                    whole[UP, k, lax.div(n, 4), lax.rem(n, 4), c].astype(jnp.float32) for c in range(2)
                ]
                at = pl.ds(pl.multiple_of(48 * n, 16), 48)
                for half in range(2):
                    both = jnp.concatenate(side(chunks[0], half) + side(chunks[1], half), axis=0)
                    out_up[at, pl.ds(WIDE * k + HALF * half, HALF)] = both.astype(jnp.bfloat16)
                return carry

            lax.fori_loop(0, 16, pair_of_chunks, 0)
            return
        for half in range(2):
            chunks = whole[part, k].astype(jnp.float32)
            tile = jnp.concatenate(side(chunks, half), axis=-2)
            (out_down, out_mixed)[part - 1][pl.ds(WIDE * k + HALF * half, HALF), :] = (
                tile.reshape(768, HALF).T.astype(jnp.bfloat16)
            )

    def keep(part, k, rows, new, state):
        if part != MIXED:
            (new_up, new_down)[part][rows, columns[k]] = new
            (state_up, state_down)[part][rows, columns[k]] = state
            return
        mixed_own[0, rows, columns[k]] = new
        mixed_own[1, rows, columns[k]] = state
        gathered["kept"] = gathered.get("kept", 0) + 1
        if gathered["kept"] == sum(piece[0] == MIXED for piece in STREAMS):
            for row, targets in enumerate(
                ((new_query, new_key, new_value, new_mixed), (state_query, state_key, state_value, state_mixed))
            ):
                everything = mixed_own[row]
                for head in range(4):
                    targets[head][...] = everything[:, 192 * head : 192 * head + 192]

    def stream(sender, part, k, first, count, axes, scatter_modes, gather_modes, lands):
        rows = pl.ds(first, count)
        copied = pl.ds(2 * first, 2 * count)
        lines = Lines(place, axes)

        def block(*index):
            return sums.at[(part, k) + index + (rows, slice(None))]

        def copy_block(*index):
            return whole.at[(part, k) + index + (copied, slice(None))]

        make_ready(part, k)
        coded, *lands = lands
        sender.scatters(0)
        yield from coded_stage(sender, lines, block, coded, lands[0])
        for stage in (1, 2):
            sender.scatters(stage)
            yield from scatter_stage(sender, lines, stage, scatter_modes[stage], block, lands[stage])
        hold(part)
        own = sums[part, k, z, y, xh, rows, :] * mean_rate
        new, state = updated(own, held[0, part, rows, columns[k]], held[1, part, rows, columns[k]])
        keep(part, k, rows, new, state)
        whole[part, k, z, y, xh, copied, :] = jnp.concatenate(
            [new[:, :HALF], new[:, HALF:]], axis=0
        ).astype(jnp.bfloat16)
        for stage in (2, 1, 0):
            sender.gathers(stage)
            yield from gather_stage(sender, lines, stage, gather_modes[stage], copy_block)
        finish(part, k, (first, count))

    def norm_stream(sender):
        loaded("norm")
        loaded("held norm")
        norm_rows[...] = jnp.zeros_like(norm_rows)
        norm_rows[1:2, 0:24] = norm_held[0]
        norm_rows[2:3, 0:24] = norm_held[1]
        placed = pltpu.roll(norm_rows[...], 24 * place.data, 1)
        norm_pair[xh, 0] = norm_grad[...]
        norm_pair[xh, 1] = placed[1:2]
        norm_pair[xh, 2] = placed[2:3]

        def share(mine, axis, size):
            arrived = sender.landing()
            sender.begin(size)
            for step in (2,) if axis == "x" else (1, 2, 3):
                sender.start(mine, mine, axis, step, arrived)
            yield
            wait_for(size, arrived)

        yield from share(norm_pair.at[xh], "x", norm_pair.at[0])
        norm_ring[0, y] = norm_pair[0] + norm_pair[1]
        yield from share(norm_ring.at[0, y], "y", norm_ring.at[0, 0:3])
        norm_ring[1, z] = norm_ring[0, 0] + norm_ring[0, 1] + norm_ring[0, 2] + norm_ring[0, 3]
        yield from share(norm_ring.at[1, z], "z", norm_ring.at[1, 0:3])
        total = norm_ring[1, 0] + norm_ring[1, 1] + norm_ring[1, 2] + norm_ring[1, 3]
        new, state = updated(total[0] * mean_rate, total[1], total[2])
        norm_all[...] = new
        norm_rows[0:1] = new
        norm_rows[1:2] = state
        own = pltpu.roll(norm_rows[...], lax.rem(768 - 24 * place.data, 768), 1)
        new_norm[...] = own[0:1, 0:24]
        state_norm[...] = own[1:2, 0:24]

    senders, streams = [], []
    first = 0
    for n, piece in enumerate(STREAMS + (None,)):
        senders.append(Sender(place, send_sems, recv_sems, (2 * n, first)))
        if piece is None:
            streams.append(norm_stream(senders[n]))
        else:
            streams.append(stream(senders[n], *piece, landings[4 * n : 4 * n + 4]))
            first += waits_of(*piece[4:])
    make_ready(UP, 0)
    pl.semaphore_wait(barrier, 7)
    for n in ORDER:
        next(streams[n], None)
    for sender in senders:
        sender.finish()


def waits_of(axes, scatter_modes, gather_modes):
    scatters = [1 + (mode == "t") for mode in scatter_modes]
    gathers = [1 + (mode == "t") for mode in gather_modes]
    again = min(gathers[2], scatters[1]) + min(gathers[1], scatters[0])
    return sum(scatters) + sum(gathers) - again


def landing_shapes():
    shapes = []
    for _, _, _, count, axes, scatter_modes, _ in STREAMS:
        lines = Lines.__new__(Lines)
        lines.axes = axes
        coded_shape = (4, 16, WIDE) if count == 24 else (3, count, WIDE)
        first_shape = (4 if axes[0] == "x" else 6,) + coded_shape
        shapes += [pltpu.VMEM(first_shape, jnp.float32)] * 2
        for stage in (1, 2):
            twice = axes[stage] != "x" and scatter_modes[stage] == "t"
            slots = 1 if axes[stage] == "x" else 6 if twice else 3
            shapes.append(pltpu.VMEM((slots,) + lines.span(stage, twice) + (count, WIDE), jnp.float32))
    return shapes


def split_kernel(up, down, mixed, norm_all, *rest):
    kept, (copy_up, copy_down, *heads, copy_norm), others, sems = rest[:14], rest[14:21], rest[21:35], rest[35]
    pairs = [(up, copy_up), (down, copy_down)]
    pairs += [(mixed.at[pl.ds(192 * n, 192), :], head) for n, head in enumerate(heads)]
    pairs += list(zip(kept, others))
    copies = [pltpu.make_async_copy(source, target, sems.at[n]) for n, (source, target) in enumerate(pairs)]
    for copy in copies:
        copy.start()
    copy_norm[...] = norm_all[0].astype(jnp.bfloat16)
    for copy in copies:
        copy.wait()


def on_device(
    grad_up, grad_down, grad_query, grad_key, grad_value, grad_mixed, grad_norm,
    weight_up, weight_down, weight_query, weight_key, weight_value, weight_mixed, weight_norm,
    moment_up, moment_down, moment_query, moment_key, moment_value, moment_mixed, moment_norm,
):
    f32, bf16 = jnp.float32, jnp.bfloat16
    anywhere = pl.BlockSpec(memory_space=pl.ANY)
    shape = jax.ShapeDtypeStruct
    operands = (
        grad_up[0].reshape(4, 4, 2, 24, 768), grad_down[0],
        grad_query[0].T, grad_key[0].T, grad_value[0].T, grad_mixed[0], grad_norm,
        weight_up, weight_down.T, weight_query, weight_key, weight_value, weight_mixed.T, weight_norm[None],
        moment_up, moment_down.T, moment_query, moment_key, moment_value, moment_mixed.T, moment_norm[None],
    )
    vmem = pl.BlockSpec(memory_space=pltpu.VMEM)
    kept_shapes = ((24, 768),) * 2 + ((24, 192),) * 4 + ((1, 24),)
    inner = (pltpu.VMEM((768, 768), bf16),) * 3 + (pltpu.VMEM((1, 768), f32),)
    inner += tuple(pltpu.VMEM(s, f32) for s in kept_shapes * 2)
    results = pl.pallas_call(
        exchange_kernel,
        name="exchange",
        out_shape=inner,
        in_specs=[anywhere] * 21,
        out_specs=[vmem] * 18,
        scratch_shapes=[
            pltpu.VMEM((3, BLOCKS) + FOLDED, f32),
            pltpu.VMEM((2, 768, 768), f32),
            pltpu.VMEM((2, 3, 24, 768), f32),
            pltpu.VMEM((2, 4, 24, 192), f32),
            pltpu.VMEM((3, BLOCKS, 4, 4, 2, 48, HALF), bf16),
            pltpu.VMEM((2, 24, 768), f32),
            pltpu.VMEM((1, 768), f32),
            pltpu.VMEM((2, 1, 24), f32),
            pltpu.VMEM((8, 768), f32),
            pltpu.VMEM((2, 3, 1, 768), f32),
            pltpu.VMEM((2, 4, 3, 1, 768), f32),
            pltpu.SemaphoreType.DMA((2 * len(STREAMS) + 2,)),
            pltpu.SemaphoreType.DMA((sum(waits_of(*piece[4:]) for piece in STREAMS) + 3,)),
            pltpu.SemaphoreType.DMA((15,)),
        ]
        + landing_shapes(),
        compiler_params=pltpu.CompilerParams(
            collective_id=0, has_side_effects=True, vmem_limit_bytes=56 * 2**20
        ),
    )(*operands)
    outs = pl.pallas_call(
        split_kernel,
        name="split",
        out_shape=(shape((768, 768), bf16),) * 2
        + (shape((192, 768), bf16),) * 4
        + (shape((768,), bf16),)
        + tuple(shape(s, f32) for s in kept_shapes * 2),
        in_specs=[vmem] * 18,
        out_specs=[anywhere] * 6 + [vmem] + [anywhere] * 14,
        scratch_shapes=[pltpu.SemaphoreType.DMA((20,))],
        compiler_params=pltpu.CompilerParams(vmem_limit_bytes=8 * 2**20),
    )(*results)
    copy_up, copy_down, copy_query, copy_key, copy_value, copy_mixed, copy_norm = outs[:7]

    def as_given(seven):
        up, down, query, key, value, mixed, norm = seven
        return (up, down.T, query, key, value, mixed.T, norm[0])

    return (
        (copy_up, copy_down, copy_query.T, copy_key.T, copy_value.T, copy_mixed, copy_norm)
        + as_given(outs[7:14])
        + as_given(outs[14:])
    )


def solution(mesh):
    return jax.shard_map(
        on_device,
        mesh=mesh,
        in_specs=(
            P("data", None, "width"),
            P("data", "width", None),
            P("data", None, "width"),
            P("data", None, "width"),
            P("data", None, "width"),
            P("data", "width", None),
            P("data", None),
        )
        + (
            P("data", "width"),
            P("width", "data"),
            P("data", "width"),
            P("data", "width"),
            P("data", "width"),
            P("width", "data"),
            P("data"),
        )
        * 2,
        out_specs=(
            P(None, "width"),
            P("width", None),
            P(None, "width"),
            P(None, "width"),
            P(None, "width"),
            P("width", None),
            P(),
        )
        + (
            P("data", "width"),
            P("width", "data"),
            P("data", "width"),
            P("data", "width"),
            P("data", "width"),
            P("width", "data"),
            P("data"),
        )
        * 2,
        check_vma=False,
    )
```
